512 devices in a mesh: tm: 16 (over y, x), space: 32 (over z, core).
Axes of the slice: x: 4, y: 4, z: 16, core: 2. Of those that a mesh axis runs over, the one named last changes fastest.
Arguments:
- initial_state: float32 [3, 768, 256], P(None, 'space'), may hold values from -2 to 2
- c_guess: float32 [16, 3, 768, 256], P('tm', None, 'space'), may hold values from -2 to 2
- friction: float32 [768, 256], P('space'), may hold values from 0.05 to 1
Outputs:
- c_points: float32 [16, 3, 768, 256], P('tm', None, 'space')
- f_points: float32 [16, 3, 768, 256], P('tm', None, 'space')
The draws below stay inside these ranges and needn't reach their ends.
All inputs are finite; a program needn't handle non-finite values.
Results may differ from the reference program's by a relative error of at most 0.00012.
Values sent between devices are 32-bit elements; how exact they have to be, the bound alone decides.
A program may use at most 64 MiB of HBM per device.

```python
import math
import jax
import jax.numpy as jnp
from jax import lax

NY = 256
STEPS = 8
NT = 16
NX = 768


def block_levels(rng, dims, shards, low, high):
    gain, own = 1.0, jax.random.fold_in(rng, 6)
    for dim, parts in shards:
        heights = jnp.exp(jax.random.uniform(jax.random.fold_in(own, dim), (parts,), jnp.float32, low / len(shards), high / len(shards)))
        gain = gain * jnp.repeat(heights, dims[dim] // parts).reshape([-1 if axis == dim else 1 for axis in range(len(dims))])
    return gain


def scatter_about(rng, shape, deviation, bound, pieces=(), kind=jnp.bfloat16):
    values = deviation * jax.random.normal(rng, shape, jnp.float32)
    if pieces:
        values = values * block_levels(rng, shape, pieces, -0.22, 0.18)
    return jnp.clip(values, -bound, bound).astype(kind)


def setup_inputs(seed: int = 0) -> dict:
    streams_of = jax.random.split(jax.random.key(seed), 4)
    initial_state = scatter_about(streams_of[0], (3, NX, NY), 0.15, 2.0, ((1, 32),), jnp.float32)
    c_guess = scatter_about(streams_of[1], (NT, 3, NX, NY), 0.15, 2.0, ((0, 16), (2, 32)), jnp.float32)
    friction = jnp.clip(jnp.exp(math.log(1.0) - 2.9957323 * jax.random.uniform(streams_of[2], (NX, NY), jnp.float32) ** block_levels(streams_of[2], (NX, NY), ((0, 32),), -0.2, 0.2)), 0.05, 1.0)
    return {"initial_state": initial_state, "c_guess": c_guess, "friction": friction}


gravity = 2.0
coriolis = 0.5
viscosity = 0.5
time_step = 0.04


def roll_neighbours(field):
    return (jnp.roll(field, -1, 0), jnp.roll(field, 1, 0), jnp.roll(field, -1, 1), jnp.roll(field, 1, 1), field)


def spread(near):
    return near[0] + near[1] + near[2] + near[3] - 4.0 * near[4]


def tendency(fields, drag, neighbours):
    height = fields[0]
    row_vel = fields[1]
    col_vel = fields[2]
    height_near = neighbours(height)
    row_near = neighbours(row_vel)
    col_near = neighbours(col_vel)
    flux_row = neighbours((1.0 + height) * row_vel)
    flux_col = neighbours((1.0 + height) * col_vel)
    row_mid = row_near[4]
    col_mid = col_near[4]
    rate_height = -(0.5 * (flux_row[0] - flux_row[1]) + 0.5 * (flux_col[2] - flux_col[3])) + viscosity * spread(height_near)
    rate_row = (-(row_mid * (0.5 * (row_near[0] - row_near[1])) + col_mid * (0.5 * (row_near[2] - row_near[3])))
                - gravity * (0.5 * (height_near[0] - height_near[1])) + coriolis * col_mid - drag * row_mid
                + viscosity * spread(row_near))
    rate_col = (-(row_mid * (0.5 * (col_near[0] - col_near[1])) + col_mid * (0.5 * (col_near[2] - col_near[3])))
                - gravity * (0.5 * (height_near[2] - height_near[3])) - coriolis * row_mid - drag * col_mid
                + viscosity * spread(col_near))
    return jnp.stack([rate_height, rate_row, rate_col])


def heun_step(fields, drag, size):
    slope_one = tendency(fields, drag, roll_neighbours)
    midpoint = fields + size * slope_one
    slope_two = tendency(midpoint, drag, roll_neighbours)
    return fields + (0.5 * size) * (slope_one + slope_two)


def reference(initial_state, c_guess, friction):
    coarse_step = STEPS * time_step

    def advance(fields, step_count):
        def inner(turn, moving):
            return heun_step(moving, friction, time_step)
        return lax.fori_loop(0, step_count, inner, fields)

    def earlier(stack):
        return jnp.concatenate([initial_state[None], stack[:-1]], 0)

    relaxed = lax.map(lambda fields: advance(fields, STEPS), earlier(c_guess))
    defect = lax.map(lambda fields: advance(fields, STEPS) - heun_step(fields, friction, coarse_step), earlier(relaxed))

    def chain(carried, defect_now):
        result = heun_step(carried, friction, coarse_step) + defect_now
        return result, result

    unused, c_points = lax.scan(chain, initial_state, defect)
    f_points = lax.map(lambda fields: advance(fields, STEPS - 1), earlier(c_points))
    return c_points, f_points
```

```python
import functools

import jax
import jax.numpy as jnp
from jax import lax
from jax.experimental import pallas as pl
from jax.experimental.pallas import tpu as pltpu
from jax.sharding import PartitionSpec as P

STEPS = 8
time_step = 0.04
coarse_step = STEPS * time_step
MESH = pl.DeviceIdType.MESH

HALO = 16
LANES = 128
BASE = 8
LOOK = 3


def shifted_lanes(pair, by, edge):
    turned = [pltpu.roll(part, by % LANES, 1) for part in pair]
    return [jnp.where(edge, turned[1], turned[0]), jnp.where(edge, turned[0], turned[1])]


def advanced(src, drag, row, scale, weight, low_edge, high_edge):
    alpha = weight * scale
    here, below, above, right, left = [], [], [], [], []
    for field in range(3):
        here.append([src[field, half, pl.ds(row, 8), :] for half in (0, 1)])
        below.append([src[field, half, pl.ds(row + 1, 8), :] for half in (0, 1)])
        above.append([src[field, half, pl.ds(row - 1, 8), :] for half in (0, 1)])
        right.append(shifted_lanes(here[field], -1, high_edge))
        left.append(shifted_lanes(here[field], 1, low_edge))
    out = [[], [], []]
    for half in (0, 1):
        e, u, w = (here[field][half] for field in range(3))
        e_ip, u_ip, w_ip = (below[field][half] for field in range(3))
        e_im, u_im, w_im = (above[field][half] for field in range(3))
        e_jp, u_jp, w_jp = (right[field][half] for field in range(3))
        e_jm, u_jm, w_jm = (left[field][half] for field in range(3))
        along = (e_ip - (1.0 + e_ip) * u_ip) + (e_im + (1.0 + e_im) * u_im)
        across = (e_jp - (1.0 + e_jp) * w_jp) + (e_jm + (1.0 + e_jm) * w_jm)
        out[0].append((weight - 4.0 * alpha) * e + alpha * (along + across))
        au = alpha * u
        aw = alpha * w
        u_low, u_high, w_low, w_high = alpha - au, alpha + au, alpha - aw, alpha + aw
        keep = drag[half, pl.ds(row, 8), :]
        out[1].append(
            (u_ip * u_low + u_im * u_high)
            + (u_jp * w_low + u_jm * w_high)
            + ((aw - (2.0 * alpha) * (e_ip - e_im)) + keep * u)
        )
        out[2].append(
            (w_ip * u_low + w_im * u_high)
            + (w_jp * w_low + w_jm * w_high)
            + (keep * w - (au + (2.0 * alpha) * (e_jp - e_jm)))
        )
    return out, here


def kernel(
    times, strips, rows,
    init_ref, guess_ref, fric_ref, c_ref, f_ref,
    first, second, third, fourth, mid, drag_raw, drags, gained, defects, own_defect, coarse_end,
    halo_send, halo_recv, fric_send, fric_recv, init_send, start_recv, own_recv,
    second_send, second_recv, defect_send, defect_recv, edge_send, edge_recv,
    hand_send, fourth_send, fourth_recv,
):
    half = times // 2
    t = lax.axis_index("tm")
    z = lax.axis_index("space")
    up = lax.rem(z + strips - 1, strips)
    down = lax.rem(z + 1, strips)
    group = t // half
    place = lax.rem(t, half)
    slot = lax.rem(t + 2, times)
    slot_group = slot // half
    slot_place = lax.rem(slot, half)

    own = pl.ds(BASE + HALO, rows)
    upper = pl.ds(BASE, HALO)
    lower = pl.ds(BASE + HALO + rows, HALO)
    own_first = pl.ds(BASE + HALO, HALO)
    own_last = pl.ds(BASE + rows, HALO)

    def remote(src, dst, send, recv, target):
        return pltpu.make_async_remote_copy(
            src_ref=src, dst_ref=dst, send_sem=send, recv_sem=recv, device_id=target, device_id_type=MESH
        )

    def edges_of(ref, send, recv):
        return (
            remote(ref.at[:, :, own_last, :], ref.at[:, :, upper, :], send.at[0], recv.at[0], (t, down)),
            remote(ref.at[:, :, own_first, :], ref.at[:, :, lower, :], send.at[1], recv.at[1], (t, up)),
        )

    barrier = pltpu.get_barrier_semaphore()

    def greet(*target):
        pl.semaphore_signal(barrier, inc=1, device_id=target, device_id_type=MESH)

    greet(t, up)
    greet(t, down)
    for other in range(1, times):
        greet(lax.rem(t + other, times), z)

    @pl.when(t == half - 1)
    def _():
        for later in range(half, times):
            greet(later, up)
            greet(later, down)

    @pl.when(t >= half)
    def _():
        greet(half - 1, up)
        greet(half - 1, down)

    is_last = t == times - 1
    for field in range(3):
        for side in (0, 1):
            cols = slice(side * LANES, (side + 1) * LANES)
            first[field, side, own, :] = jnp.where(is_last, init_ref[field, :, cols], guess_ref[0, field, :, cols])
    for side in (0, 1):
        drag_raw[0, side, own, :] = fric_ref[:, side * LANES : (side + 1) * LANES]

    @pl.when(t < half)
    def _():
        for field in range(3):
            for side in (0, 1):
                third[field, side, own, :] = init_ref[field, :, side * LANES : (side + 1) * LANES]

    greeted = jnp.where(t == half - 1, 2 * half, jnp.where(t >= half, 2, 0))
    pl.semaphore_wait(barrier, times + 1 + greeted)

    first_edges = edges_of(first, halo_send, halo_recv)
    drag_edges = edges_of(drag_raw, fric_send, fric_recv)
    third_edges = edges_of(third, init_send, start_recv)
    for copy in first_edges + drag_edges:
        copy.start()

    @pl.when(t < half)
    def _():
        for copy in third_edges:
            copy.start()

    lane = lax.broadcasted_iota(jnp.int32, (8, LANES), 1)
    low_edge = lane == 0
    high_edge = lane == LANES - 1
    full = range(BASE, BASE + 2 * HALO + rows, 8)
    inner = range(BASE + 8, BASE + 2 * HALO + rows - 8, 8)
    strip = range(BASE + HALO, BASE + HALO + rows, 8)

    def half_step(state, kind, step, chunks):
        for row in chunks:
            values, _ = advanced(state, drags.at[kind], row, 0.5 * step, 1.0, low_edge, high_edge)
            for field in range(3):
                for side in (0, 1):
                    mid[field, side, pl.ds(row, 8), :] = values[field][side]

    def end_step(state, kind, step, chunks, put):
        for row in chunks:
            values, _ = advanced(mid, drags.at[kind + 1], row, 0.5 * step, 0.5, low_edge, high_edge)
            for field in range(3):
                for side in (0, 1):
                    put(field, side, row, values[field][side] + 0.5 * state[field, side, pl.ds(row, 8), :])

    def heun(state, kind, step, chunks, put):
        half_step(state, kind, step, chunks)
        end_step(state, kind, step, chunks if put is not None else chunks, put)

    def fine_steps(state, count, chunks):
        def put(field, side, row, value):
            state[field, side, pl.ds(row, 8), :] = value

        def step(_, carry):
            heun(state, 0, time_step, chunks, put)
            return carry

        lax.fori_loop(0, count, step, 0)

    for copy in first_edges + drag_edges:
        copy.wait()
    for row in full:
        for side in (0, 1):
            base = 2.0 * drag_raw[0, side, pl.ds(row, 8), :] + 4.0
            for kind, step in ((0, time_step), (2, coarse_step)):
                drags[kind, side, pl.ds(row, 8), :] = 1.0 - (0.5 * step) * base
                drags[kind + 1, side, pl.ds(row, 8), :] = 0.5 - (0.25 * step) * base

    fine_steps(first, STEPS - 4, full)
    fine_steps(first, 4, inner)

    is_first = t == times - 2
    for field in range(3):
        for side in (0, 1):
            second[field, side, own, :] = jnp.where(
                is_first, init_ref[field, :, side * LANES : (side + 1) * LANES], first[field, side, own, :]
            )
    second_edges = edges_of(second, second_send, second_recv)
    for copy in second_edges:
        copy.start()
    for copy in second_edges:
        copy.wait_recv()

    half_step(second, 2, coarse_step, inner)

    def put_gain(field, side, row, value):
        gained[field, side, pl.ds(row - BASE - HALO, 8), :] = value

    end_step(second, 2, coarse_step, strip, put_gain)
    for copy in second_edges:
        copy.wait_send()
    fine_steps(second, STEPS - 4, full)
    fine_steps(second, 4, inner)
    own_defect[...] = second[:, :, own, :] - gained[...]

    d_own = pl.ds(HALO, rows)

    def defect_copy(turn):
        target = slot_group * half + half - 1 - turn
        return remote(
            own_defect,
            defects.at[slot_place, :, :, d_own, :],
            defect_send.at[turn],
            defect_recv.at[slot_place],
            (target, z),
        )

    def send_defect(turn, carry):
        defect_copy(turn).start()
        return carry

    lax.fori_loop(0, half - slot_place, send_defect, 0)

    def edge_copies(turn):
        return (
            remote(
                defects.at[turn, :, :, pl.ds(rows, HALO), :],
                defects.at[turn, :, :, pl.ds(0, HALO), :],
                edge_send.at[0, turn], edge_recv.at[0, turn], (t, down),
            ),
            remote(
                defects.at[turn, :, :, pl.ds(HALO, HALO), :],
                defects.at[turn, :, :, pl.ds(HALO + rows, HALO), :],
                edge_send.at[1, turn], edge_recv.at[1, turn], (t, up),
            ),
        )

    def pass_edges(turn, carry):
        remote(
            own_defect, defects.at[turn, :, :, d_own, :], defect_send.at[turn], defect_recv.at[turn], (t, z)
        ).wait_recv()
        for copy in edge_copies(turn):
            copy.start()
        return carry

    ahead = jnp.minimum(jnp.where(t < half, LOOK, half), place + 1)
    lax.fori_loop(0, ahead, pass_edges, 0)

    @pl.when(t >= half)
    def _():
        remote(coarse_end, third.at[:, :, own, :], init_send.at[0], own_recv, (t, z)).wait_recv()

    for copy in third_edges:
        copy.wait_recv()

    def coarse(turn, chunks):
        for copy in edge_copies(turn):
            copy.wait_recv()

        def put(field, side, row, value):
            third[field, side, pl.ds(row, 8), :] = value + defects[turn, field, side, pl.ds(row - BASE, 8), :]

        half_step(third, 2, coarse_step, chunks)
        end_step(third, 2, coarse_step, chunks, put)

    def chain(chunks):
        def step(turn, carry):
            @pl.when(turn + ahead <= place)
            def _():
                pass_edges(turn + ahead, 0)

            coarse(turn, chunks)
            return carry

        return step

    @pl.when(t < half)
    def _():
        for copy in third_edges:
            copy.wait_send()

    middle = jnp.minimum(place, half // 2)
    lax.fori_loop(0, middle, chain(full), 0)
    lax.fori_loop(middle, place, chain(inner), 0)

    fourth[:, :, own, :] = third[:, :, own, :]
    fourth_edges = edges_of(fourth, fourth_send, fourth_recv)
    for copy in fourth_edges:
        copy.start()

    for copy in edge_copies(place):
        copy.wait_recv()

    def put_end(field, side, row, value):
        value = value + defects[place, field, side, pl.ds(row - BASE, 8), :]
        coarse_end[field, side, pl.ds(row - BASE - HALO, 8), :] = value
        c_ref[0, field, pl.ds(row - BASE - HALO, 8), side * LANES : (side + 1) * LANES] = value

    half_step(third, 2, coarse_step, inner)
    end_step(third, 2, coarse_step, strip, put_end)

    def hand_copies(turn):
        target = times - 1 - turn
        return (
            remote(coarse_end, third.at[:, :, own, :], hand_send.at[0, turn], own_recv, (target, z)),
            remote(
                coarse_end.at[:, :, pl.ds(rows - HALO, HALO), :], third.at[:, :, upper, :],
                hand_send.at[1, turn], start_recv.at[0], (target, down),
            ),
            remote(
                coarse_end.at[:, :, pl.ds(0, HALO), :], third.at[:, :, lower, :],
                hand_send.at[2, turn], start_recv.at[1], (target, up),
            ),
        )

    @pl.when(t == half - 1)
    def _():
        def hand(turn, carry):
            for copy in hand_copies(turn):
                copy.start()
            return carry

        lax.fori_loop(0, half, hand, 0)

    for copy in fourth_edges:
        copy.wait()
    fine_steps(fourth, STEPS - 5, full)
    fine_steps(fourth, 4, inner)
    for field in range(3):
        for side in (0, 1):
            f_ref[0, field, :, side * LANES : (side + 1) * LANES] = fourth[field, side, own, :]

    def sent_defect(turn, carry):
        defect_copy(turn).wait_send()
        return carry

    lax.fori_loop(0, half - slot_place, sent_defect, 0)

    def sent_edges(turn, carry):
        for copy in edge_copies(turn):
            copy.wait_send()
        return carry

    lax.fori_loop(0, place + 1, sent_edges, 0)

    @pl.when(t == half - 1)
    def _():
        def handed(turn, carry):
            for copy in hand_copies(turn):
                copy.wait_send()
            return carry

        lax.fori_loop(0, half, handed, 0)


def solution(mesh):
    times, strips = mesh.shape["tm"], mesh.shape["space"]
    half = times // 2

    def body(initial_state, c_guess, friction):
        rows = friction.shape[0]
        tall = BASE + 2 * HALO + rows + 8
        state = pltpu.VMEM((3, 2, tall, LANES), jnp.float32)
        part = pltpu.VMEM((3, 2, rows, LANES), jnp.float32)
        dma = pltpu.SemaphoreType.DMA
        vmem = pl.BlockSpec(memory_space=pltpu.VMEM)
        shape = jax.ShapeDtypeStruct(c_guess.shape, jnp.float32)
        return pl.pallas_call(
            functools.partial(kernel, times, strips, rows),
            out_shape=(shape, shape),
            in_specs=[vmem] * 3,
            out_specs=(vmem, vmem),
            scratch_shapes=[
                state, state, state, state, state,
                pltpu.VMEM((1, 2, tall, LANES), jnp.float32),
                pltpu.VMEM((4, 2, tall, LANES), jnp.float32),
                part,
                pltpu.VMEM((half, 3, 2, 2 * HALO + rows, LANES), jnp.float32),
                part,
                part,
                dma((2,)), dma((2,)), dma((2,)), dma((2,)), dma((2,)), dma((2,)), dma,
                dma((2,)), dma((2,)), dma((half,)), dma((half,)), dma((2, half)), dma((2, half)),
                dma((3, half)), dma((2,)), dma((2,)),
            ],
            compiler_params=pltpu.CompilerParams(collective_id=0, has_side_effects=True),
            cost_estimate=pl.CostEstimate(flops=100_000_000, bytes_accessed=1_000_000, transcendentals=0),
        )(initial_state, c_guess, friction)

    return jax.shard_map(
        body,
        mesh=mesh,
        in_specs=(P(None, "space", None), P("tm", None, "space", None), P("space", None)),
        out_specs=(P("tm", None, "space", None), P("tm", None, "space", None)),
        check_vma=False,
    )
```

```python
import functools

import jax
import jax.numpy as jnp
from jax import lax
from jax.experimental import pallas as pl
from jax.experimental.pallas import tpu as pltpu
from jax.sharding import PartitionSpec as P

STEPS = 8
time_step = 0.04
coarse_step = STEPS * time_step
MESH = pl.DeviceIdType.MESH

HALO = 16
LANES = 128
BASE = 8
LOOK = 3


def shifted_lanes(pair, by, edge):
    turned = [pltpu.roll(part, by % LANES, 1) for part in pair]
    return [jnp.where(edge, turned[1], turned[0]), jnp.where(edge, turned[0], turned[1])]


def advanced(src, drag, row, scale, weight, low_edge, high_edge):
    alpha = weight * scale
    here, below, above, right, left = [], [], [], [], []
    for field in range(3):
        here.append([src[field, half, pl.ds(row, 8), :] for half in (0, 1)])
        below.append([src[field, half, pl.ds(row + 1, 8), :] for half in (0, 1)])
        above.append([src[field, half, pl.ds(row - 1, 8), :] for half in (0, 1)])
        right.append(shifted_lanes(here[field], -1, high_edge))
        left.append(shifted_lanes(here[field], 1, low_edge))
    out = [[], [], []]
    for half in (0, 1):
        e, u, w = (here[field][half] for field in range(3))
        e_ip, u_ip, w_ip = (below[field][half] for field in range(3))
        e_im, u_im, w_im = (above[field][half] for field in range(3))
        e_jp, u_jp, w_jp = (right[field][half] for field in range(3))
        e_jm, u_jm, w_jm = (left[field][half] for field in range(3))
        along = (e_ip - (1.0 + e_ip) * u_ip) + (e_im + (1.0 + e_im) * u_im)
        across = (e_jp - (1.0 + e_jp) * w_jp) + (e_jm + (1.0 + e_jm) * w_jm)
        out[0].append((weight - 4.0 * alpha) * e + alpha * (along + across))
        au = alpha * u
        aw = alpha * w
        u_low, u_high, w_low, w_high = alpha - au, alpha + au, alpha - aw, alpha + aw
        keep = drag[half, pl.ds(row, 8), :]
        out[1].append(
            (u_ip * u_low + u_im * u_high)
            + (u_jp * w_low + u_jm * w_high)
            + ((aw - (2.0 * alpha) * (e_ip - e_im)) + keep * u)
        )
        out[2].append(
            (w_ip * u_low + w_im * u_high)
            + (w_jp * w_low + w_jm * w_high)
            + (keep * w - (au + (2.0 * alpha) * (e_jp - e_jm)))
        )
    return out, here


def kernel(
    times, strips, rows,
    init_ref, guess_ref, fric_ref, c_ref, f_ref,
    first, second, third, fourth, mid, drag_raw, drags, gained, defects, own_defect,
    halo_send, halo_recv, fric_send, fric_recv, init_send, start_recv,
    second_send, second_recv, defect_send, defect_recv, edge_send, edge_recv,
    fourth_send, fourth_recv,
):
    half = times // 2
    t = lax.axis_index("tm")
    z = lax.axis_index("space")
    up = lax.rem(z + strips - 1, strips)
    down = lax.rem(z + 1, strips)
    slot = lax.rem(t + 2, times)

    own = pl.ds(BASE + HALO, rows)
    upper = pl.ds(BASE, HALO)
    lower = pl.ds(BASE + HALO + rows, HALO)
    own_first = pl.ds(BASE + HALO, HALO)
    own_last = pl.ds(BASE + rows, HALO)

    def remote(src, dst, send, recv, target):
        return pltpu.make_async_remote_copy(
            src_ref=src, dst_ref=dst, send_sem=send, recv_sem=recv, device_id=target, device_id_type=MESH
        )

    def edges_of(ref, send, recv):
        return (
            remote(ref.at[:, :, own_last, :], ref.at[:, :, upper, :], send.at[0], recv.at[0], (t, down)),
            remote(ref.at[:, :, own_first, :], ref.at[:, :, lower, :], send.at[1], recv.at[1], (t, up)),
        )

    barrier = pltpu.get_barrier_semaphore()

    def greet(*target):
        pl.semaphore_signal(barrier, inc=1, device_id=target, device_id_type=MESH)

    greet(t, up)
    greet(t, down)
    for other in range(1, times):
        greet(lax.rem(t + other, times), z)

    is_last = t == times - 1
    for field in range(3):
        for side in (0, 1):
            cols = slice(side * LANES, (side + 1) * LANES)
            first[field, side, own, :] = jnp.where(is_last, init_ref[field, :, cols], guess_ref[0, field, :, cols])
    for side in (0, 1):
        drag_raw[0, side, own, :] = fric_ref[:, side * LANES : (side + 1) * LANES]

    for field in range(3):
        for side in (0, 1):
            third[0, field, side, own, :] = init_ref[field, :, side * LANES : (side + 1) * LANES]

    pl.semaphore_wait(barrier, times + 1)

    first_edges = edges_of(first, halo_send, halo_recv)
    drag_edges = edges_of(drag_raw, fric_send, fric_recv)
    third_edges = edges_of(third.at[0], init_send.at[0], start_recv.at[0])
    later_edges = edges_of(third.at[1], init_send.at[1], start_recv.at[1])
    for copy in first_edges + drag_edges + third_edges:
        copy.start()

    lane = lax.broadcasted_iota(jnp.int32, (8, LANES), 1)
    low_edge = lane == 0
    high_edge = lane == LANES - 1
    full = range(BASE, BASE + 2 * HALO + rows, 8)
    inner = range(BASE + 8, BASE + 2 * HALO + rows - 8, 8)
    strip = range(BASE + HALO, BASE + HALO + rows, 8)

    def half_step(state, kind, step, chunks):
        for row in chunks:
            values, _ = advanced(state, drags.at[kind], row, 0.5 * step, 1.0, low_edge, high_edge)
            for field in range(3):
                for side in (0, 1):
                    mid[field, side, pl.ds(row, 8), :] = values[field][side]

    def end_step(state, kind, step, chunks, put):
        for row in chunks:
            values, _ = advanced(mid, drags.at[kind + 1], row, 0.5 * step, 0.5, low_edge, high_edge)
            for field in range(3):
                for side in (0, 1):
                    put(field, side, row, values[field][side] + 0.5 * state[field, side, pl.ds(row, 8), :])

    def heun(state, kind, step, chunks, put):
        half_step(state, kind, step, chunks)
        end_step(state, kind, step, chunks if put is not None else chunks, put)

    def fine_steps(state, count, chunks):
        def put(field, side, row, value):
            state[field, side, pl.ds(row, 8), :] = value

        def step(_, carry):
            heun(state, 0, time_step, chunks, put)
            return carry

        lax.fori_loop(0, count, step, 0)

    for copy in first_edges + drag_edges:
        copy.wait()
    for row in full:
        for side in (0, 1):
            base = 2.0 * drag_raw[0, side, pl.ds(row, 8), :] + 4.0
            for kind, step in ((0, time_step), (2, coarse_step)):
                drags[kind, side, pl.ds(row, 8), :] = 1.0 - (0.5 * step) * base
                drags[kind + 1, side, pl.ds(row, 8), :] = 0.5 - (0.25 * step) * base

    fine_steps(first, STEPS - 4, full)
    fine_steps(first, 4, inner)

    is_first = t == times - 2
    for field in range(3):
        for side in (0, 1):
            second[field, side, own, :] = jnp.where(
                is_first, init_ref[field, :, side * LANES : (side + 1) * LANES], first[field, side, own, :]
            )
    second_edges = edges_of(second, second_send, second_recv)
    for copy in second_edges:
        copy.start()
    for copy in second_edges:
        copy.wait_recv()

    half_step(second, 2, coarse_step, inner)

    def put_gain(field, side, row, value):
        gained[field, side, pl.ds(row - BASE - HALO, 8), :] = value

    end_step(second, 2, coarse_step, strip, put_gain)
    for copy in second_edges:
        copy.wait_send()
    fine_steps(second, STEPS - 4, full)
    fine_steps(second, 4, inner)
    own_defect[...] = second[:, :, own, :] - gained[...]

    d_own = pl.ds(HALO, rows)

    def defect_copy(turn):
        target = times - 1 - turn
        return remote(
            own_defect, defects.at[slot, :, :, d_own, :], defect_send.at[turn], defect_recv.at[slot], (target, z)
        )

    def each_defect(act):
        def one(turn, carry):
            @pl.when(times - 1 - turn != t)
            def _():
                act(defect_copy(turn))

            return carry

        lax.fori_loop(0, times - slot, one, 0)

    each_defect(lambda copy: copy.start())

    @pl.when(t >= times - 2)
    def _():
        defects[slot, :, :, d_own, :] = own_defect[...]

    def each_edge(turn, act):
        need = 2 * (half - 1 - lax.rem(turn, half))

        def copies(count):
            return (
                remote(
                    defects.at[turn, :, :, pl.ds(HALO + rows - count, count), :],
                    defects.at[turn, :, :, pl.ds(HALO - count, count), :],
                    edge_send.at[0, turn], edge_recv.at[0, turn], (t, down),
                ),
                remote(
                    defects.at[turn, :, :, pl.ds(HALO, count), :],
                    defects.at[turn, :, :, pl.ds(HALO + rows, count), :],
                    edge_send.at[1, turn], edge_recv.at[1, turn], (t, up),
                ),
            )

        @pl.when(need > 8)
        def _():
            for copy in copies(16):
                act(copy)

        @pl.when((need > 0) & (need <= 8))
        def _():
            for copy in copies(8):
                act(copy)

    def pass_edges(turn, carry):
        @pl.when(turn != slot)
        def _():
            remote(
                own_defect, defects.at[turn, :, :, d_own, :], defect_send.at[turn], defect_recv.at[turn], (t, z)
            ).wait_recv()

        each_edge(turn, lambda copy: copy.start())
        return carry

    ahead = jnp.minimum(LOOK, t + 1)
    lax.fori_loop(0, ahead, pass_edges, 0)

    for copy in third_edges:
        copy.wait()

    def chain(state, chunks):
        def step(turn, carry):
            @pl.when(turn + ahead <= t)
            def _():
                pass_edges(turn + ahead, 0)

            half_step(state, 2, coarse_step, chunks)
            each_edge(turn, lambda copy: copy.wait_recv())

            def put(field, side, row, value):
                state[field, side, pl.ds(row, 8), :] = value + defects[turn, field, side, pl.ds(row - BASE, 8), :]

            end_step(state, 2, coarse_step, chunks, put)
            return carry

        return step

    wide = max(half - 4, 0)
    lax.fori_loop(0, jnp.minimum(t, wide), chain(third.at[0], full), 0)
    lax.fori_loop(wide, jnp.minimum(t, half), chain(third.at[0], inner), 0)

    @pl.when(t >= half)
    def _():
        third[1, :, :, own, :] = third[0, :, :, own, :]
        for copy in later_edges:
            copy.start()
        for copy in later_edges:
            copy.wait()
        lax.fori_loop(half, jnp.minimum(t, half + wide), chain(third.at[1], full), 0)
        lax.fori_loop(half + wide, t, chain(third.at[1], inner), 0)

    state = third.at[t // half]
    fourth[:, :, own, :] = state[:, :, own, :]
    fourth_edges = edges_of(fourth, fourth_send, fourth_recv)
    for copy in fourth_edges:
        copy.start()

    def put_end(field, side, row, value):
        c_ref[0, field, pl.ds(row - BASE - HALO, 8), side * LANES : (side + 1) * LANES] = (
            value + defects[t, field, side, pl.ds(row - BASE, 8), :]
        )

    half_step(state, 2, coarse_step, inner)
    each_edge(t, lambda copy: copy.wait_recv())
    end_step(state, 2, coarse_step, strip, put_end)

    for copy in fourth_edges:
        copy.wait()
    fine_steps(fourth, STEPS - 5, full)
    fine_steps(fourth, 4, inner)
    for field in range(3):
        for side in (0, 1):
            f_ref[0, field, :, side * LANES : (side + 1) * LANES] = fourth[field, side, own, :]

    each_defect(lambda copy: copy.wait_send())

    def sent_edges(turn, carry):
        each_edge(turn, lambda copy: copy.wait_send())
        return carry

    lax.fori_loop(0, t + 1, sent_edges, 0)


def solution(mesh):
    times, strips = mesh.shape["tm"], mesh.shape["space"]

    def body(initial_state, c_guess, friction):
        rows = friction.shape[0]
        tall = BASE + 2 * HALO + rows + 8
        state = pltpu.VMEM((3, 2, tall, LANES), jnp.float32)
        part = pltpu.VMEM((3, 2, rows, LANES), jnp.float32)
        dma = pltpu.SemaphoreType.DMA
        vmem = pl.BlockSpec(memory_space=pltpu.VMEM)
        shape = pltpu.VMEM(c_guess.shape, jnp.float32)
        return pl.pallas_call(
            functools.partial(kernel, times, strips, rows),
            out_shape=(shape, shape),
            in_specs=[vmem] * 3,
            out_specs=(vmem, vmem),
            scratch_shapes=[
                state, state,
                pltpu.VMEM((2, 3, 2, tall, LANES), jnp.float32),
                state, state,
                pltpu.VMEM((1, 2, tall, LANES), jnp.float32),
                pltpu.VMEM((4, 2, tall, LANES), jnp.float32),
                part,
                pltpu.VMEM((times, 3, 2, 2 * HALO + rows, LANES), jnp.float32),
                part,
                dma((2,)), dma((2,)), dma((2,)), dma((2,)), dma((2, 2)), dma((2, 2)),
                dma((2,)), dma((2,)), dma((times,)), dma((times,)), dma((2, times)), dma((2, times)),
                dma((2,)), dma((2,)),
            ],
            compiler_params=pltpu.CompilerParams(collective_id=0, has_side_effects=True),
            cost_estimate=pl.CostEstimate(flops=100_000_000, bytes_accessed=1_000_000, transcendentals=0),
        )(initial_state, c_guess, friction)

    return jax.shard_map(
        body,
        mesh=mesh,
        in_specs=(P(None, "space", None), P("tm", None, "space", None), P("space", None)),
        out_specs=(P("tm", None, "space", None), P("tm", None, "space", None)),
        check_vma=False,
    )
```

```python
import functools
import math

import jax
import jax.numpy as jnp
from jax import lax
from jax.experimental import pallas as pl
from jax.experimental.pallas import tpu as pltpu
from jax.sharding import PartitionSpec as P

STEPS = 8
time_step = 0.04
coarse_step = STEPS * time_step
MESH = pl.DeviceIdType.MESH

HALO = 16
LANES = 128
BASE = 8


def shifted_lanes(pair, by, edge):
    turned = [pltpu.roll(part, by % LANES, 1) for part in pair]
    return [jnp.where(edge, turned[1], turned[0]), jnp.where(edge, turned[0], turned[1])]


def advanced(src, drag, row, scale, weight, low_edge, high_edge):
    alpha = weight * scale
    here, below, above, right, left = [], [], [], [], []
    for field in range(3):
        here.append([src[field, half, pl.ds(row, 8), :] for half in (0, 1)])
        below.append([src[field, half, pl.ds(row + 1, 8), :] for half in (0, 1)])
        above.append([src[field, half, pl.ds(row - 1, 8), :] for half in (0, 1)])
        right.append(shifted_lanes(here[field], -1, high_edge))
        left.append(shifted_lanes(here[field], 1, low_edge))
    out = [[], [], []]
    for half in (0, 1):
        e, u, w = (here[field][half] for field in range(3))
        e_ip, u_ip, w_ip = (below[field][half] for field in range(3))
        e_im, u_im, w_im = (above[field][half] for field in range(3))
        e_jp, u_jp, w_jp = (right[field][half] for field in range(3))
        e_jm, u_jm, w_jm = (left[field][half] for field in range(3))
        along = (e_ip - (1.0 + e_ip) * u_ip) + (e_im + (1.0 + e_im) * u_im)
        across = (e_jp - (1.0 + e_jp) * w_jp) + (e_jm + (1.0 + e_jm) * w_jm)
        out[0].append((weight - 4.0 * alpha) * e + alpha * (along + across))
        au = alpha * u
        aw = alpha * w
        u_low, u_high, w_low, w_high = alpha - au, alpha + au, alpha - aw, alpha + aw
        keep = drag[half, pl.ds(row, 8), :]
        out[1].append(
            (u_ip * u_low + u_im * u_high)
            + (u_jp * w_low + u_jm * w_high)
            + ((aw - (2.0 * alpha) * (e_ip - e_im)) + keep * u)
        )
        out[2].append(
            (w_ip * u_low + w_im * u_high)
            + (w_jp * w_low + w_jm * w_high)
            + (keep * w - (au + (2.0 * alpha) * (e_jp - e_jm)))
        )
    return out, here


def kernel(
    times, strips, rows,
    init_ref, guess_ref, fric_ref, c_ref, f_ref,
    first, second, third, fourth, mid, drag_raw, drags, gained, defects, own_defect,
    halo_send, halo_recv, fric_send, fric_recv, init_send, start_recv,
    second_send, second_recv, defect_send, defect_recv, edge_send, edge_recv,
    fourth_send, fourth_recv, hand_send, hand_recv,
):
    half = times // 2
    span = math.isqrt(times)
    t = lax.axis_index("tm")
    z = lax.axis_index("space")
    up = lax.rem(z + strips - 1, strips)
    down = lax.rem(z + 1, strips)
    place = lax.rem(t, half)
    slot = lax.rem(t + 2, times)
    slot_place = lax.rem(slot, half)
    hands = (t >= half - span) & (t < half)
    last = jnp.where(hands, half - 1, place)
    slot_end = slot // half * half + half
    slot_low = jnp.where(slot < half, jnp.minimum(slot, half - span), slot)
    handed = half // span

    own = pl.ds(BASE + HALO, rows)
    upper = pl.ds(BASE, HALO)
    lower = pl.ds(BASE + HALO + rows, HALO)
    own_first = pl.ds(BASE + HALO, HALO)
    own_last = pl.ds(BASE + rows, HALO)

    def remote(src, dst, send, recv, target):
        return pltpu.make_async_remote_copy(
            src_ref=src, dst_ref=dst, send_sem=send, recv_sem=recv, device_id=target, device_id_type=MESH
        )

    def edges_of(ref, send, recv):
        return (
            remote(ref.at[:, :, own_last, :], ref.at[:, :, upper, :], send.at[0], recv.at[0], (t, down)),
            remote(ref.at[:, :, own_first, :], ref.at[:, :, lower, :], send.at[1], recv.at[1], (t, up)),
        )

    barrier = pltpu.get_barrier_semaphore()

    def greet(*target):
        pl.semaphore_signal(barrier, inc=1, device_id=target, device_id_type=MESH)

    greet(t, up)
    greet(t, down)
    for other in range(1, times):
        greet(lax.rem(t + other, times), z)

    @pl.when(hands)
    def _():
        for turn in range(1, handed + 1):
            greet(t + turn * span, up)
            greet(t + turn * span, down)

    @pl.when(t >= half)
    def _():
        giver = half - span + lax.rem(t, span)
        greet(giver, up)
        greet(giver, down)

    is_last = t == times - 1
    for field in range(3):
        for side in (0, 1):
            cols = slice(side * LANES, (side + 1) * LANES)
            first[field, side, own, :] = jnp.where(is_last, init_ref[field, :, cols], guess_ref[0, field, :, cols])
    for side in (0, 1):
        drag_raw[0, side, own, :] = fric_ref[:, side * LANES : (side + 1) * LANES]

    @pl.when(t < half)
    def _():
        for field in range(3):
            for part in (0, 1):
                third[field, part, own, :] = init_ref[field, :, part * LANES : (part + 1) * LANES]

    greeted = jnp.where(hands, 2 * handed, jnp.where(t >= half, 2, 0))
    pl.semaphore_wait(barrier, times + 1 + greeted)

    first_edges = edges_of(first, halo_send, halo_recv)
    drag_edges = edges_of(drag_raw, fric_send, fric_recv)
    third_edges = edges_of(third, init_send, start_recv)
    for copy in first_edges + drag_edges:
        copy.start()

    @pl.when(t < half)
    def _():
        for copy in third_edges:
            copy.start()

    lane = lax.broadcasted_iota(jnp.int32, (8, LANES), 1)
    low_edge = lane == 0
    high_edge = lane == LANES - 1
    full = range(BASE, BASE + 2 * HALO + rows, 8)
    inner = range(BASE + 8, BASE + 2 * HALO + rows - 8, 8)
    strip = range(BASE + HALO, BASE + HALO + rows, 8)

    def half_step(state, kind, step, chunks):
        for row in chunks:
            values, _ = advanced(state, drags.at[kind], row, 0.5 * step, 1.0, low_edge, high_edge)
            for field in range(3):
                for side in (0, 1):
                    mid[field, side, pl.ds(row, 8), :] = values[field][side]

    def end_step(state, kind, step, chunks, put):
        for row in chunks:
            values, _ = advanced(mid, drags.at[kind + 1], row, 0.5 * step, 0.5, low_edge, high_edge)
            for field in range(3):
                for side in (0, 1):
                    put(field, side, row, values[field][side] + 0.5 * state[field, side, pl.ds(row, 8), :])

    def heun(state, kind, step, chunks, put):
        half_step(state, kind, step, chunks)
        end_step(state, kind, step, chunks if put is not None else chunks, put)

    def fine_steps(state, count, chunks):
        def put(field, side, row, value):
            state[field, side, pl.ds(row, 8), :] = value

        def step(_, carry):
            heun(state, 0, time_step, chunks, put)
            return carry

        lax.fori_loop(0, count, step, 0)

    for copy in first_edges + drag_edges:
        copy.wait()
    for row in full:
        for side in (0, 1):
            base = 2.0 * drag_raw[0, side, pl.ds(row, 8), :] + 4.0
            for kind, step in ((0, time_step), (2, coarse_step)):
                drags[kind, side, pl.ds(row, 8), :] = 1.0 - (0.5 * step) * base
                drags[kind + 1, side, pl.ds(row, 8), :] = 0.5 - (0.25 * step) * base

    fine_steps(first, STEPS - 4, full)
    fine_steps(first, 4, inner)

    is_first = t == times - 2
    for field in range(3):
        for side in (0, 1):
            second[field, side, own, :] = jnp.where(
                is_first, init_ref[field, :, side * LANES : (side + 1) * LANES], first[field, side, own, :]
            )
    second_edges = edges_of(second, second_send, second_recv)
    for copy in second_edges:
        copy.start()
    for copy in second_edges:
        copy.wait_recv()

    half_step(second, 2, coarse_step, inner)

    def put_gain(field, side, row, value):
        gained[field, side, pl.ds(row - BASE - HALO, 8), :] = value

    end_step(second, 2, coarse_step, strip, put_gain)
    for copy in second_edges:
        copy.wait_send()
    fine_steps(second, STEPS - 4, full)
    fine_steps(second, 4, inner)
    own_defect[...] = second[:, :, own, :] - gained[...]

    d_own = pl.ds(HALO, rows)

    def each_defect(act):
        def one(turn, carry):
            target = slot_end - 1 - turn

            @pl.when(target != t)
            def _():
                act(
                    remote(
                        own_defect, defects.at[slot_place, :, :, d_own, :],
                        defect_send.at[turn], defect_recv.at[slot_place], (target, z),
                    )
                )

            return carry

        lax.fori_loop(0, slot_end - slot_low, one, 0)

    each_defect(lambda copy: copy.start())
    keeps = (t >= slot_low) & (t < slot_end)

    @pl.when(keeps)
    def _():
        defects[slot_place, :, :, d_own, :] = own_defect[...]

    def each_edge(turn, act):
        need = 2 * (half - 1 - turn)

        def copies(count):
            return (
                remote(
                    defects.at[turn, :, :, pl.ds(HALO + rows - count, count), :],
                    defects.at[turn, :, :, pl.ds(HALO - count, count), :],
                    edge_send.at[0, turn], edge_recv.at[0, turn], (t, down),
                ),
                remote(
                    defects.at[turn, :, :, pl.ds(HALO, count), :],
                    defects.at[turn, :, :, pl.ds(HALO + rows, count), :],
                    edge_send.at[1, turn], edge_recv.at[1, turn], (t, up),
                ),
            )

        @pl.when(need > 8)
        def _():
            for copy in copies(16):
                act(copy)

        @pl.when((need > 0) & (need <= 8))
        def _():
            for copy in copies(8):
                act(copy)

    def pass_edges(turn, carry):
        @pl.when(jnp.logical_not(keeps & (turn == slot_place)))
        def _():
            remote(
                own_defect, defects.at[turn, :, :, d_own, :], defect_send.at[turn], defect_recv.at[turn], (t, z)
            ).wait_recv()

        each_edge(turn, lambda copy: copy.start())
        return carry

    lax.fori_loop(0, last + 1, pass_edges, 0)

    @pl.when(t < half)
    def _():
        for copy in third_edges:
            copy.wait_send()

    @pl.when(t >= half)
    def _():
        remote(third.at[:, :, own, :], third.at[:, :, own, :], hand_send.at[0, 0], hand_recv, (t, z)).wait_recv()

    for copy in third_edges:
        copy.wait_recv()

    def chain(chunks):
        def step(turn, carry):
            half_step(third, 2, coarse_step, chunks)
            each_edge(turn, lambda copy: copy.wait_recv())

            def put(field, part, row, value):
                third[field, part, pl.ds(row, 8), :] = value + defects[turn, field, part, pl.ds(row - BASE, 8), :]

            end_step(third, 2, coarse_step, chunks, put)
            return carry

        return step

    wide = max(half - 4, 0)
    lax.fori_loop(0, jnp.minimum(place, wide), chain(full), 0)
    lax.fori_loop(wide, place, chain(inner), 0)

    fourth[:, :, own, :] = third[:, :, own, :]
    fourth_edges = edges_of(fourth, fourth_send, fourth_recv)
    for copy in fourth_edges:
        copy.start()

    def put_out():
        for field in range(3):
            for part in (0, 1):
                c_ref[0, field, :, part * LANES : (part + 1) * LANES] = third[field, part, own, :]

    chain(inner)(place, 0)
    put_out()
    lax.fori_loop(place + 1, last + 1, chain(inner), 0)

    def each_hand(act):
        def one(turn, carry):
            target = t + span * turn + span
            act(remote(third.at[:, :, own, :], third.at[:, :, own, :], hand_send.at[0, turn], hand_recv, (target, z)))
            act(
                remote(
                    third.at[:, :, own_last, :], third.at[:, :, upper, :],
                    hand_send.at[1, turn], start_recv.at[0], (target, down),
                )
            )
            act(
                remote(
                    third.at[:, :, own_first, :], third.at[:, :, lower, :],
                    hand_send.at[2, turn], start_recv.at[1], (target, up),
                )
            )
            return carry

        lax.fori_loop(0, handed, one, 0)

    @pl.when(hands)
    def _():
        each_hand(lambda copy: copy.start())

    for copy in fourth_edges:
        copy.wait()
    fine_steps(fourth, STEPS - 5, full)
    fine_steps(fourth, 4, inner)
    for field in range(3):
        for side in (0, 1):
            f_ref[0, field, :, side * LANES : (side + 1) * LANES] = fourth[field, side, own, :]

    each_defect(lambda copy: copy.wait_send())

    def sent_edges(turn, carry):
        each_edge(turn, lambda copy: copy.wait_send())
        return carry

    lax.fori_loop(0, last + 1, sent_edges, 0)

    @pl.when(hands)
    def _():
        each_hand(lambda copy: copy.wait_send())


def solution(mesh):
    times, strips = mesh.shape["tm"], mesh.shape["space"]

    def body(initial_state, c_guess, friction):
        rows = friction.shape[0]
        tall = BASE + 2 * HALO + rows + 8
        state = pltpu.VMEM((3, 2, tall, LANES), jnp.float32)
        part = pltpu.VMEM((3, 2, rows, LANES), jnp.float32)
        dma = pltpu.SemaphoreType.DMA
        vmem = pl.BlockSpec(memory_space=pltpu.VMEM)
        shape = pltpu.VMEM(c_guess.shape, jnp.float32)
        return pl.pallas_call(
            functools.partial(kernel, times, strips, rows),
            out_shape=(shape, shape),
            in_specs=[vmem] * 3,
            out_specs=(vmem, vmem),
            scratch_shapes=[
                state, state,
                state, state, state,
                pltpu.VMEM((1, 2, tall, LANES), jnp.float32),
                pltpu.VMEM((4, 2, tall, LANES), jnp.float32),
                part,
                pltpu.VMEM((times // 2, 3, 2, 2 * HALO + rows, LANES), jnp.float32),
                part,
                dma((2,)), dma((2,)), dma((2,)), dma((2,)), dma((2,)), dma((2,)),
                dma((2,)), dma((2,)), dma((times,)), dma((times,)), dma((2, times)), dma((2, times)),
                dma((2,)), dma((2,)), dma((3, 4)), dma,
            ],
            compiler_params=pltpu.CompilerParams(collective_id=0, has_side_effects=True),
            cost_estimate=pl.CostEstimate(flops=100_000_000, bytes_accessed=1_000_000, transcendentals=0),
        )(initial_state, c_guess, friction)

    return jax.shard_map(
        body,
        mesh=mesh,
        in_specs=(P(None, "space", None), P("tm", None, "space", None), P("space", None)),
        out_specs=(P("tm", None, "space", None), P("tm", None, "space", None)),
        check_vma=False,
    )
```

```python
import functools
import math

import jax
import jax.numpy as jnp
from jax import lax
from jax.experimental import pallas as pl
from jax.experimental.pallas import tpu as pltpu
from jax.sharding import PartitionSpec as P

STEPS = 8
time_step = 0.04
coarse_step = STEPS * time_step
MESH = pl.DeviceIdType.MESH

HALO = 16
LANES = 128
BASE = 8


def shifted_lanes(pair, by, edge):
    turned = [pltpu.roll(part, by % LANES, 1) for part in pair]
    return [jnp.where(edge, turned[1], turned[0]), jnp.where(edge, turned[0], turned[1])]


def advanced(src, drag, row, scale, weight, low_edge, high_edge):
    alpha = weight * scale
    here, below, above, right, left = [], [], [], [], []
    for field in range(3):
        here.append([src[field, half, pl.ds(row, 8), :] for half in (0, 1)])
        below.append([src[field, half, pl.ds(row + 1, 8), :] for half in (0, 1)])
        above.append([src[field, half, pl.ds(row - 1, 8), :] for half in (0, 1)])
        right.append(shifted_lanes(here[field], -1, high_edge))
        left.append(shifted_lanes(here[field], 1, low_edge))
    out = [[], [], []]
    for half in (0, 1):
        e, u, w = (here[field][half] for field in range(3))
        e_ip, u_ip, w_ip = (below[field][half] for field in range(3))
        e_im, u_im, w_im = (above[field][half] for field in range(3))
        e_jp, u_jp, w_jp = (right[field][half] for field in range(3))
        e_jm, u_jm, w_jm = (left[field][half] for field in range(3))
        along = (e_ip - (1.0 + e_ip) * u_ip) + (e_im + (1.0 + e_im) * u_im)
        across = (e_jp - (1.0 + e_jp) * w_jp) + (e_jm + (1.0 + e_jm) * w_jm)
        out[0].append((weight - 4.0 * alpha) * e + alpha * (along + across))
        au = alpha * u
        aw = alpha * w
        u_low, u_high, w_low, w_high = alpha - au, alpha + au, alpha - aw, alpha + aw
        keep = drag[half, pl.ds(row, 8), :]
        out[1].append(
            (u_ip * u_low + u_im * u_high)
            + (u_jp * w_low + u_jm * w_high)
            + ((aw - (2.0 * alpha) * (e_ip - e_im)) + keep * u)
        )
        out[2].append(
            (w_ip * u_low + w_im * u_high)
            + (w_jp * w_low + w_jm * w_high)
            + (keep * w - (au + (2.0 * alpha) * (e_jp - e_jm)))
        )
    return out, here


def kernel(
    times, strips, rows,
    init_ref, guess_ref, fric_ref, c_ref, f_ref,
    first, second, third, fourth, mid, drag_raw, drags, gained, defects, own_defect,
    halo_send, halo_recv, fric_send, fric_recv, init_send, start_recv,
    second_send, second_recv, defect_send, defect_recv, edge_send, edge_recv,
    fourth_send, fourth_recv, hand_send, hand_recv, share_send, met,
):
    half = times // 2
    span = math.isqrt(times)
    t = lax.axis_index("tm")
    z = lax.axis_index("space")
    up = lax.rem(z + strips - 1, strips)
    down = lax.rem(z + 1, strips)
    place = lax.rem(t, half)
    slot = lax.rem(t + 2, times)
    slot_place = lax.rem(slot, half)
    hands = (t >= half - span) & (t < half)
    last = jnp.where(hands, half - 1, place)
    slot_end = slot // half * half + half
    slot_low = jnp.where(slot < half, jnp.minimum(slot, half - span), slot)
    handed = half // span

    own = pl.ds(BASE + HALO, rows)
    upper = pl.ds(BASE, HALO)
    lower = pl.ds(BASE + HALO + rows, HALO)
    own_first = pl.ds(BASE + HALO, HALO)
    own_last = pl.ds(BASE + rows, HALO)

    def remote(src, dst, send, recv, target):
        return pltpu.make_async_remote_copy(
            src_ref=src, dst_ref=dst, send_sem=send, recv_sem=recv, device_id=target, device_id_type=MESH
        )

    def edges_of(ref, send, recv):
        return (
            remote(ref.at[:, :, own_last, :], ref.at[:, :, upper, :], send.at[0], recv.at[0], (t, down)),
            remote(ref.at[:, :, own_first, :], ref.at[:, :, lower, :], send.at[1], recv.at[1], (t, up)),
        )

    barrier = pltpu.get_barrier_semaphore()

    def greet(*target):
        pl.semaphore_signal(barrier, inc=1, device_id=target, device_id_type=MESH)

    greet(t, up)
    greet(t, down)
    partners = []
    for bit in range((times - 1).bit_length()):
        far = 1 << bit
        partners.append(t + far - 2 * far * lax.rem(t // far, 2))
    for partner in partners:
        greet(partner, z)

    is_last = t == times - 1
    for field in range(3):
        for side in (0, 1):
            cols = slice(side * LANES, (side + 1) * LANES)
            first[field, side, own, :] = jnp.where(is_last, init_ref[field, :, cols], guess_ref[0, field, :, cols])
    for side in (0, 1):
        drag_raw[0, side, own, :] = fric_ref[:, side * LANES : (side + 1) * LANES]

    @pl.when(t < half)
    def _():
        for field in range(3):
            for part in (0, 1):
                third[field, part, own, :] = init_ref[field, :, part * LANES : (part + 1) * LANES]

    pl.semaphore_wait(barrier, 2 + len(partners))

    def tell(turn):
        pl.semaphore_signal(met.at[turn], inc=1, device_id=(partners[turn], z), device_id_type=MESH)

    def hear(turn):
        pl.semaphore_wait(met.at[turn], 1)

    tell(0)
    first_edges = edges_of(first, halo_send, halo_recv)
    drag_edges = edges_of(drag_raw, fric_send, fric_recv)
    third_edges = edges_of(third, init_send, start_recv)
    for copy in first_edges + drag_edges:
        copy.start()

    @pl.when(t < half)
    def _():
        for copy in third_edges:
            copy.start()

    lane = lax.broadcasted_iota(jnp.int32, (8, LANES), 1)
    low_edge = lane == 0
    high_edge = lane == LANES - 1
    full = range(BASE, BASE + 2 * HALO + rows, 8)
    inner = range(BASE + 8, BASE + 2 * HALO + rows - 8, 8)
    strip = range(BASE + HALO, BASE + HALO + rows, 8)

    def half_step(state, kind, step, chunks):
        for row in chunks:
            values, _ = advanced(state, drags.at[kind], row, 0.5 * step, 1.0, low_edge, high_edge)
            for field in range(3):
                for side in (0, 1):
                    mid[field, side, pl.ds(row, 8), :] = values[field][side]

    def end_step(state, kind, step, chunks, put):
        for row in chunks:
            values, _ = advanced(mid, drags.at[kind + 1], row, 0.5 * step, 0.5, low_edge, high_edge)
            for field in range(3):
                for side in (0, 1):
                    put(field, side, row, values[field][side] + 0.5 * state[field, side, pl.ds(row, 8), :])

    def heun(state, kind, step, chunks, put):
        half_step(state, kind, step, chunks)
        end_step(state, kind, step, chunks if put is not None else chunks, put)

    def fine_steps(state, count, chunks):
        def put(field, side, row, value):
            state[field, side, pl.ds(row, 8), :] = value

        def step(_, carry):
            heun(state, 0, time_step, chunks, put)
            return carry

        lax.fori_loop(0, count, step, 0)

    for copy in first_edges + drag_edges:
        copy.wait()
    for row in full:
        for side in (0, 1):
            base = 2.0 * drag_raw[0, side, pl.ds(row, 8), :] + 4.0
            for kind, step in ((0, time_step), (2, coarse_step)):
                drags[kind, side, pl.ds(row, 8), :] = 1.0 - (0.5 * step) * base
                drags[kind + 1, side, pl.ds(row, 8), :] = 0.5 - (0.25 * step) * base

    hear(0)
    if len(partners) > 1:
        tell(1)

    fine_steps(first, STEPS - 4, full)
    fine_steps(first, 4, inner)

    is_first = t == times - 2
    for field in range(3):
        for side in (0, 1):
            second[field, side, own, :] = jnp.where(
                is_first, init_ref[field, :, side * LANES : (side + 1) * LANES], first[field, side, own, :]
            )
    second_edges = edges_of(second, second_send, second_recv)
    for copy in second_edges:
        copy.start()
    if len(partners) > 1:
        hear(1)
    if len(partners) > 2:
        tell(2)
    for copy in second_edges:
        copy.wait_recv()

    half_step(second, 2, coarse_step, inner)

    def put_gain(field, side, row, value):
        gained[field, side, pl.ds(row - BASE - HALO, 8), :] = value

    end_step(second, 2, coarse_step, strip, put_gain)
    if len(partners) > 2:
        hear(2)
    if len(partners) > 3:
        tell(3)
    for copy in second_edges:
        copy.wait_send()
    fine_steps(second, STEPS - 4, full)
    fine_steps(second, 4, inner)
    own_defect[...] = second[:, :, own, :] - gained[...]

    if len(partners) > 3:
        hear(3)
    d_own = pl.ds(HALO, rows)

    def each_defect(act):
        def one(turn, carry):
            target = slot_end - 1 - turn

            @pl.when(target != t)
            def _():
                act(
                    remote(
                        own_defect, defects.at[slot_place, :, :, d_own, :],
                        defect_send.at[turn], defect_recv.at[slot_place], (target, z),
                    )
                )

            return carry

        lax.fori_loop(0, slot_end - slot_low, one, 0)

    each_defect(lambda copy: copy.start())
    keeps = (t >= slot_low) & (t < slot_end)

    @pl.when(keeps)
    def _():
        defects[slot_place, :, :, d_own, :] = own_defect[...]

    def each_edge(turn, act):
        need = 2 * (half - 1 - turn)

        def copies(count):
            return (
                remote(
                    defects.at[turn, :, :, pl.ds(HALO + rows - count, count), :],
                    defects.at[turn, :, :, pl.ds(HALO - count, count), :],
                    edge_send.at[0, turn], edge_recv.at[0, turn], (t, down),
                ),
                remote(
                    defects.at[turn, :, :, pl.ds(HALO, count), :],
                    defects.at[turn, :, :, pl.ds(HALO + rows, count), :],
                    edge_send.at[1, turn], edge_recv.at[1, turn], (t, up),
                ),
            )

        @pl.when(need > 8)
        def _():
            for copy in copies(16):
                act(copy)

        @pl.when((need > 0) & (need <= 8))
        def _():
            for copy in copies(8):
                act(copy)

    def pass_edges(turn, carry):
        @pl.when(jnp.logical_not(keeps & (turn == slot_place)))
        def _():
            remote(
                own_defect, defects.at[turn, :, :, d_own, :], defect_send.at[turn], defect_recv.at[turn], (t, z)
            ).wait_recv()

        each_edge(turn, lambda copy: copy.start())
        return carry

    lax.fori_loop(0, last + 1, pass_edges, 0)

    upper_core = lax.rem(z, 2) == 0
    share_down = remote(third.at[:, :, own_last, :], third.at[:, :, upper, :], share_send, start_recv.at[0], (t, down))
    share_up = remote(third.at[:, :, own_first, :], third.at[:, :, lower, :], share_send, start_recv.at[1], (t, up))

    @pl.when(t < half)
    def _():
        for copy in third_edges:
            copy.wait_send()

    @pl.when(t >= half)
    def _():
        remote(third.at[:, :, own, :], third.at[:, :, own, :], hand_send.at[0, 0], hand_recv, (t, z)).wait_recv()

        @pl.when(upper_core)
        def _():
            share_down.start()

        @pl.when(jnp.logical_not(upper_core))
        def _():
            share_up.start()

    for copy in third_edges:
        copy.wait_recv()

    @pl.when((t >= half) & upper_core)
    def _():
        share_down.wait_send()

    @pl.when((t >= half) & jnp.logical_not(upper_core))
    def _():
        share_up.wait_send()

    def chain(chunks):
        def step(turn, carry):
            half_step(third, 2, coarse_step, chunks)
            each_edge(turn, lambda copy: copy.wait_recv())

            def put(field, part, row, value):
                third[field, part, pl.ds(row, 8), :] = value + defects[turn, field, part, pl.ds(row - BASE, 8), :]

            end_step(third, 2, coarse_step, chunks, put)
            return carry

        return step

    wide = max(half - 4, 0)
    lax.fori_loop(0, jnp.minimum(place, wide), chain(full), 0)
    lax.fori_loop(wide, place, chain(inner), 0)

    fourth[:, :, own, :] = third[:, :, own, :]
    fourth_edges = edges_of(fourth, fourth_send, fourth_recv)
    for copy in fourth_edges:
        copy.start()

    def put_out():
        for field in range(3):
            for part in (0, 1):
                c_ref[0, field, :, part * LANES : (part + 1) * LANES] = third[field, part, own, :]

    chain(inner)(place, 0)
    put_out()
    lax.fori_loop(place + 1, last + 1, chain(inner), 0)

    def each_hand(act):
        def one(turn, carry):
            target = t + span * turn + span
            act(remote(third.at[:, :, own, :], third.at[:, :, own, :], hand_send.at[0, turn], hand_recv, (target, z)))

            @pl.when(upper_core)
            def _():
                act(
                    remote(
                        third.at[:, :, own_first, :], third.at[:, :, lower, :],
                        hand_send.at[1, turn], start_recv.at[1], (target, up),
                    )
                )

            @pl.when(jnp.logical_not(upper_core))
            def _():
                act(
                    remote(
                        third.at[:, :, own_last, :], third.at[:, :, upper, :],
                        hand_send.at[1, turn], start_recv.at[0], (target, down),
                    )
                )

            return carry

        lax.fori_loop(0, handed, one, 0)

    @pl.when(hands)
    def _():
        each_hand(lambda copy: copy.start())

    for copy in fourth_edges:
        copy.wait()
    fine_steps(fourth, STEPS - 5, full)
    fine_steps(fourth, 4, inner)
    for field in range(3):
        for side in (0, 1):
            f_ref[0, field, :, side * LANES : (side + 1) * LANES] = fourth[field, side, own, :]

    each_defect(lambda copy: copy.wait_send())

    def sent_edges(turn, carry):
        each_edge(turn, lambda copy: copy.wait_send())
        return carry

    lax.fori_loop(0, last + 1, sent_edges, 0)

    @pl.when(hands)
    def _():
        each_hand(lambda copy: copy.wait_send())


def solution(mesh):
    times, strips = mesh.shape["tm"], mesh.shape["space"]

    def body(initial_state, c_guess, friction):
        rows = friction.shape[0]
        tall = BASE + 2 * HALO + rows + 8
        state = pltpu.VMEM((3, 2, tall, LANES), jnp.float32)
        part = pltpu.VMEM((3, 2, rows, LANES), jnp.float32)
        dma = pltpu.SemaphoreType.DMA
        vmem = pl.BlockSpec(memory_space=pltpu.VMEM)
        shape = pltpu.VMEM(c_guess.shape, jnp.float32)
        return pl.pallas_call(
            functools.partial(kernel, times, strips, rows),
            out_shape=(shape, shape),
            in_specs=[vmem] * 3,
            out_specs=(vmem, vmem),
            scratch_shapes=[
                state, state,
                state, state, state,
                pltpu.VMEM((1, 2, tall, LANES), jnp.float32),
                pltpu.VMEM((4, 2, tall, LANES), jnp.float32),
                part,
                pltpu.VMEM((times // 2, 3, 2, 2 * HALO + rows, LANES), jnp.float32),
                part,
                dma((2,)), dma((2,)), dma((2,)), dma((2,)), dma((2,)), dma((2,)),
                dma((2,)), dma((2,)), dma((times,)), dma((times,)), dma((2, times)), dma((2, times)),
                dma((2,)), dma((2,)), dma((2, 4)), dma, dma,
                pltpu.SemaphoreType.REGULAR((4,)),
            ],
            compiler_params=pltpu.CompilerParams(collective_id=0, has_side_effects=True),
            cost_estimate=pl.CostEstimate(flops=100_000_000, bytes_accessed=1_000_000, transcendentals=0),
        )(initial_state, c_guess, friction)

    return jax.shard_map(
        body,
        mesh=mesh,
        in_specs=(P(None, "space", None), P("tm", None, "space", None), P("space", None)),
        out_specs=(P("tm", None, "space", None), P("tm", None, "space", None)),
        check_vma=False,
    )
```

```python
import functools
import math

import jax
import jax.numpy as jnp
from jax import lax
from jax.experimental import pallas as pl
from jax.experimental.pallas import tpu as pltpu
from jax.sharding import PartitionSpec as P

STEPS = 8
time_step = 0.04
coarse_step = STEPS * time_step
MESH = pl.DeviceIdType.MESH

HALO = 16
LANES = 128
BASE = 8


def shifted_lanes(pair, by, edge):
    turned = [pltpu.roll(part, by % LANES, 1) for part in pair]
    return [jnp.where(edge, turned[1], turned[0]), jnp.where(edge, turned[0], turned[1])]


def advanced(src, drag, row, scale, weight, low_edge, high_edge):
    alpha = weight * scale
    here, below, above, right, left = [], [], [], [], []
    for field in range(3):
        here.append([src[field, half, pl.ds(row, 8), :] for half in (0, 1)])
        below.append([src[field, half, pl.ds(row + 1, 8), :] for half in (0, 1)])
        above.append([src[field, half, pl.ds(row - 1, 8), :] for half in (0, 1)])
        right.append(shifted_lanes(here[field], -1, high_edge))
        left.append(shifted_lanes(here[field], 1, low_edge))
    out = [[], [], []]
    for half in (0, 1):
        e, u, w = (here[field][half] for field in range(3))
        e_ip, u_ip, w_ip = (below[field][half] for field in range(3))
        e_im, u_im, w_im = (above[field][half] for field in range(3))
        e_jp, u_jp, w_jp = (right[field][half] for field in range(3))
        e_jm, u_jm, w_jm = (left[field][half] for field in range(3))
        along = (e_ip - (1.0 + e_ip) * u_ip) + (e_im + (1.0 + e_im) * u_im)
        across = (e_jp - (1.0 + e_jp) * w_jp) + (e_jm + (1.0 + e_jm) * w_jm)
        out[0].append((weight - 4.0 * alpha) * e + alpha * (along + across))
        au = alpha * u
        aw = alpha * w
        u_low, u_high, w_low, w_high = alpha - au, alpha + au, alpha - aw, alpha + aw
        keep = drag[half, pl.ds(row, 8), :]
        out[1].append(
            (u_ip * u_low + u_im * u_high)
            + (u_jp * w_low + u_jm * w_high)
            + ((aw - (2.0 * alpha) * (e_ip - e_im)) + keep * u)
        )
        out[2].append(
            (w_ip * u_low + w_im * u_high)
            + (w_jp * w_low + w_jm * w_high)
            + (keep * w - (au + (2.0 * alpha) * (e_jp - e_jm)))
        )
    return out, here


def kernel(
    times, strips, rows,
    init_ref, guess_ref, fric_ref, c_ref, f_ref,
    first, second, third, fourth, mid, drag_raw, drags, gained, defects, own_defect,
    halo_send, halo_recv, fric_send, fric_recv, init_send, start_recv,
    second_send, second_recv, defect_send, defect_recv, edge_send, edge_recv,
    fourth_send, fourth_recv, hand_send, hand_recv, share_send, met, load_sem,
):
    half = times // 2
    span = math.isqrt(times)
    t = lax.axis_index("tm")
    z = lax.axis_index("space")
    up = lax.rem(z + strips - 1, strips)
    down = lax.rem(z + 1, strips)
    place = lax.rem(t, half)
    slot = lax.rem(t + 2, times)
    slot_place = lax.rem(slot, half)
    hands = t < span
    last = jnp.where(hands, half - 1, place)
    slot_end = slot // half * half + half
    handed = half // span

    own = pl.ds(BASE + HALO, rows)
    upper = pl.ds(BASE, HALO)
    lower = pl.ds(BASE + HALO + rows, HALO)
    own_first = pl.ds(BASE + HALO, HALO)
    own_last = pl.ds(BASE + rows, HALO)

    def remote(src, dst, send, recv, target):
        return pltpu.make_async_remote_copy(
            src_ref=src, dst_ref=dst, send_sem=send, recv_sem=recv, device_id=target, device_id_type=MESH
        )

    def edges_of(ref, send, recv):
        return (
            remote(ref.at[:, :, own_last, :], ref.at[:, :, upper, :], send.at[0], recv.at[0], (t, down)),
            remote(ref.at[:, :, own_first, :], ref.at[:, :, lower, :], send.at[1], recv.at[1], (t, up)),
        )

    barrier = pltpu.get_barrier_semaphore()

    def greet(*target):
        pl.semaphore_signal(barrier, inc=1, device_id=target, device_id_type=MESH)

    greet(t, up)
    greet(t, down)
    partners = []
    for bit in range((times - 1).bit_length()):
        far = 1 << bit
        partners.append(t + far - 2 * far * lax.rem(t // far, 2))
    for partner in partners:
        greet(partner, z)

    is_last = t == times - 1
    is_first = t == times - 2

    def loads(block, ref, turn):
        return [
            pltpu.make_async_copy(
                block.at[..., pl.ds(side * LANES, LANES)], ref.at[:, side, own, :], load_sem.at[turn, side]
            )
            for side in (0, 1)
        ]

    def each_load(act):
        @pl.when(is_last)
        def _():
            for copy in loads(init_ref, first, 0):
                act(copy)

        @pl.when(jnp.logical_not(is_last))
        def _():
            for copy in loads(guess_ref.at[0], first, 0):
                act(copy)

        for side in (0, 1):
            act(
                pltpu.make_async_copy(
                    fric_ref.at[:, pl.ds(side * LANES, LANES)], drag_raw.at[0, side, own, :], load_sem.at[1, side]
                )
            )

        @pl.when(t < half)
        def _():
            for copy in loads(init_ref, third, 2):
                act(copy)

        @pl.when(is_first)
        def _():
            for copy in loads(init_ref, second, 2):
                act(copy)

    each_load(lambda copy: copy.start())
    each_load(lambda copy: copy.wait())
    pl.semaphore_wait(barrier, 2 + len(partners))

    def tell(turn):
        pl.semaphore_signal(met.at[turn], inc=1, device_id=(partners[turn], z), device_id_type=MESH)

    def hear(turn):
        pl.semaphore_wait(met.at[turn], 1)

    tell(0)
    first_edges = edges_of(first, halo_send, halo_recv)
    drag_edges = edges_of(drag_raw, fric_send, fric_recv)
    third_edges = edges_of(third, init_send, start_recv)
    for copy in first_edges + drag_edges:
        copy.start()

    @pl.when(t < half)
    def _():
        for copy in third_edges:
            copy.start()

    lane = lax.broadcasted_iota(jnp.int32, (8, LANES), 1)
    low_edge = lane == 0
    high_edge = lane == LANES - 1
    full = range(BASE, BASE + 2 * HALO + rows, 8)
    inner = range(BASE + 8, BASE + 2 * HALO + rows - 8, 8)
    strip = range(BASE + HALO, BASE + HALO + rows, 8)

    def half_step(state, kind, step, chunks):
        for row in chunks:
            values, _ = advanced(state, drags.at[kind], row, 0.5 * step, 1.0, low_edge, high_edge)
            for field in range(3):
                for side in (0, 1):
                    mid[field, side, pl.ds(row, 8), :] = values[field][side]

    def end_step(state, kind, step, chunks, put):
        for row in chunks:
            values, _ = advanced(mid, drags.at[kind + 1], row, 0.5 * step, 0.5, low_edge, high_edge)
            for field in range(3):
                for side in (0, 1):
                    put(field, side, row, values[field][side] + 0.5 * state[field, side, pl.ds(row, 8), :])

    def heun(state, kind, step, chunks, put):
        half_step(state, kind, step, chunks)
        end_step(state, kind, step, chunks if put is not None else chunks, put)

    def fine_steps(state, count, chunks):
        def put(field, side, row, value):
            state[field, side, pl.ds(row, 8), :] = value

        def step(_, carry):
            heun(state, 0, time_step, chunks, put)
            return carry

        lax.fori_loop(0, count, step, 0)

    for copy in first_edges + drag_edges:
        copy.wait()
    for row in full:
        for side in (0, 1):
            base = 2.0 * drag_raw[0, side, pl.ds(row, 8), :] + 4.0
            for kind, step in ((0, time_step), (2, coarse_step)):
                drags[kind, side, pl.ds(row, 8), :] = 1.0 - (0.5 * step) * base
                drags[kind + 1, side, pl.ds(row, 8), :] = 0.5 - (0.25 * step) * base

    hear(0)
    if len(partners) > 1:
        tell(1)

    fine_steps(first, STEPS - 4, full)
    fine_steps(first, 4, inner)

    @pl.when(jnp.logical_not(is_first))
    def _():
        second[:, :, own, :] = first[:, :, own, :]

    second_edges = edges_of(second, second_send, second_recv)
    for copy in second_edges:
        copy.start()
    if len(partners) > 1:
        hear(1)
    if len(partners) > 2:
        tell(2)
    for copy in second_edges:
        copy.wait_recv()

    half_step(second, 2, coarse_step, inner)

    def put_gain(field, side, row, value):
        gained[field, side, pl.ds(row - BASE - HALO, 8), :] = value

    end_step(second, 2, coarse_step, strip, put_gain)
    if len(partners) > 2:
        hear(2)
    if len(partners) > 3:
        tell(3)
    for copy in second_edges:
        copy.wait_send()
    fine_steps(second, STEPS - 4, full)
    fine_steps(second, 4, inner)
    own_defect[...] = second[:, :, own, :] - gained[...]

    if len(partners) > 3:
        hear(3)
    d_own = pl.ds(HALO, rows)

    slot_low = jnp.maximum(slot, jnp.where(slot < half, span, 0))
    fronts = jnp.where(slot < half, span, 0)

    def each_defect(act):
        def one(turn, carry):
            target = jnp.where(turn < fronts, turn, slot_end - 1 - (turn - fronts))

            @pl.when(target != t)
            def _():
                act(
                    remote(
                        own_defect, defects.at[slot_place, :, :, d_own, :],
                        defect_send.at[turn], defect_recv.at[slot_place], (target, z),
                    )
                )

            return carry

        lax.fori_loop(0, fronts + slot_end - slot_low, one, 0)

    each_defect(lambda copy: copy.start())
    keeps = ((t >= slot_low) & (t < slot_end)) | (t < fronts)

    @pl.when(keeps)
    def _():
        defects[slot_place, :, :, d_own, :] = own_defect[...]

    def each_edge(turn, act):
        need = 2 * (half - 1 - turn)

        def copies(count):
            return (
                remote(
                    defects.at[turn, :, :, pl.ds(HALO + rows - count, count), :],
                    defects.at[turn, :, :, pl.ds(HALO - count, count), :],
                    edge_send.at[0, turn], edge_recv.at[0, turn], (t, down),
                ),
                remote(
                    defects.at[turn, :, :, pl.ds(HALO, count), :],
                    defects.at[turn, :, :, pl.ds(HALO + rows, count), :],
                    edge_send.at[1, turn], edge_recv.at[1, turn], (t, up),
                ),
            )

        @pl.when(need > 8)
        def _():
            for copy in copies(16):
                act(copy)

        @pl.when((need > 0) & (need <= 8))
        def _():
            for copy in copies(8):
                act(copy)

    def pass_edges(turn, carry):
        @pl.when(jnp.logical_not(keeps & (turn == slot_place)))
        def _():
            remote(
                own_defect, defects.at[turn, :, :, d_own, :], defect_send.at[turn], defect_recv.at[turn], (t, z)
            ).wait_recv()

        each_edge(turn, lambda copy: copy.start())
        return carry

    lax.fori_loop(0, last + 1, pass_edges, 0)

    upper_core = lax.rem(z, 2) == 0
    share_down = remote(third.at[:, :, own_last, :], third.at[:, :, upper, :], share_send, start_recv.at[0], (t, down))
    share_up = remote(third.at[:, :, own_first, :], third.at[:, :, lower, :], share_send, start_recv.at[1], (t, up))

    @pl.when(t < half)
    def _():
        for copy in third_edges:
            copy.wait_send()

    @pl.when(t >= half)
    def _():
        remote(third.at[:, :, own, :], third.at[:, :, own, :], hand_send.at[0, 0], hand_recv, (t, z)).wait_recv()

        @pl.when(upper_core)
        def _():
            share_down.start()

        @pl.when(jnp.logical_not(upper_core))
        def _():
            share_up.start()

    for copy in third_edges:
        copy.wait_recv()

    @pl.when((t >= half) & upper_core)
    def _():
        share_down.wait_send()

    @pl.when((t >= half) & jnp.logical_not(upper_core))
    def _():
        share_up.wait_send()

    def chain(chunks):
        def step(turn, carry):
            half_step(third, 2, coarse_step, chunks)
            each_edge(turn, lambda copy: copy.wait_recv())

            def put(field, part, row, value):
                third[field, part, pl.ds(row, 8), :] = value + defects[turn, field, part, pl.ds(row - BASE, 8), :]

            end_step(third, 2, coarse_step, chunks, put)
            return carry

        return step

    wide = max(half - 4, 0)
    lax.fori_loop(0, jnp.minimum(place, wide), chain(full), 0)
    lax.fori_loop(wide, place, chain(inner), 0)

    fourth[:, :, own, :] = third[:, :, own, :]
    fourth_edges = edges_of(fourth, fourth_send, fourth_recv)
    for copy in fourth_edges:
        copy.start()

    def put_out():
        for field in range(3):
            for part in (0, 1):
                c_ref[0, field, :, part * LANES : (part + 1) * LANES] = third[field, part, own, :]

    lax.fori_loop(place, jnp.minimum(place + 1, wide), chain(full), 0)
    lax.fori_loop(jnp.maximum(place, wide), place + 1, chain(inner), 0)
    put_out()
    lax.fori_loop(place + 1, jnp.minimum(last + 1, wide), chain(full), 0)
    lax.fori_loop(jnp.maximum(place + 1, wide), last + 1, chain(inner), 0)

    def each_hand(act):
        def one(turn, carry):
            target = t + times - span - span * turn
            act(remote(third.at[:, :, own, :], third.at[:, :, own, :], hand_send.at[0, turn], hand_recv, (target, z)))

            @pl.when(upper_core)
            def _():
                act(
                    remote(
                        third.at[:, :, own_first, :], third.at[:, :, lower, :],
                        hand_send.at[1, turn], start_recv.at[1], (target, up),
                    )
                )

            @pl.when(jnp.logical_not(upper_core))
            def _():
                act(
                    remote(
                        third.at[:, :, own_last, :], third.at[:, :, upper, :],
                        hand_send.at[1, turn], start_recv.at[0], (target, down),
                    )
                )

            return carry

        lax.fori_loop(0, handed, one, 0)

    @pl.when(hands)
    def _():
        each_hand(lambda copy: copy.start())

    for copy in fourth_edges:
        copy.wait()
    fine_steps(fourth, STEPS - 5, full)
    fine_steps(fourth, 4, inner)
    for field in range(3):
        for side in (0, 1):
            f_ref[0, field, :, side * LANES : (side + 1) * LANES] = fourth[field, side, own, :]

    each_defect(lambda copy: copy.wait_send())

    def sent_edges(turn, carry):
        each_edge(turn, lambda copy: copy.wait_send())
        return carry

    lax.fori_loop(0, last + 1, sent_edges, 0)

    @pl.when(hands)
    def _():
        each_hand(lambda copy: copy.wait_send())


def solution(mesh):
    times, strips = mesh.shape["tm"], mesh.shape["space"]

    def body(initial_state, c_guess, friction):
        rows = friction.shape[0]
        tall = BASE + 2 * HALO + rows + 8
        state = pltpu.VMEM((3, 2, tall, LANES), jnp.float32)
        part = pltpu.VMEM((3, 2, rows, LANES), jnp.float32)
        dma = pltpu.SemaphoreType.DMA
        vmem = pl.BlockSpec(memory_space=pltpu.VMEM)
        shape = pltpu.VMEM(c_guess.shape, jnp.float32)
        return pl.pallas_call(
            functools.partial(kernel, times, strips, rows),
            out_shape=(shape, shape),
            in_specs=[pl.BlockSpec(memory_space=pl.ANY)] * 3,
            out_specs=(vmem, vmem),
            scratch_shapes=[
                state, state,
                state, state, state,
                pltpu.VMEM((1, 2, tall, LANES), jnp.float32),
                pltpu.VMEM((4, 2, tall, LANES), jnp.float32),
                part,
                pltpu.VMEM((times // 2, 3, 2, 2 * HALO + rows, LANES), jnp.float32),
                part,
                dma((2,)), dma((2,)), dma((2,)), dma((2,)), dma((2,)), dma((2,)),
                dma((2,)), dma((2,)), dma((times,)), dma((times,)), dma((2, times)), dma((2, times)),
                dma((2,)), dma((2,)), dma((2, 4)), dma, dma,
                pltpu.SemaphoreType.REGULAR((4,)), dma((3, 2)),
            ],
            compiler_params=pltpu.CompilerParams(collective_id=0, has_side_effects=True),
            cost_estimate=pl.CostEstimate(flops=100_000_000, bytes_accessed=1_000_000, transcendentals=0),
        )(initial_state, c_guess, friction)

    return jax.shard_map(
        body,
        mesh=mesh,
        in_specs=(P(None, "space", None), P("tm", None, "space", None), P("space", None)),
        out_specs=(P("tm", None, "space", None), P("tm", None, "space", None)),
        check_vma=False,
    )
```

```python
import functools
import math

import jax
import jax.numpy as jnp
from jax import lax
from jax.experimental import pallas as pl
from jax.experimental.pallas import tpu as pltpu
from jax.sharding import PartitionSpec as P

STEPS = 8
time_step = 0.04
coarse_step = STEPS * time_step
MESH = pl.DeviceIdType.MESH

HALO = 16
LANES = 128
BASE = 8


def shifted_lanes(pair, by, edge):
    turned = [pltpu.roll(part, by % LANES, 1) for part in pair]
    return [jnp.where(edge, turned[1], turned[0]), jnp.where(edge, turned[0], turned[1])]


def advanced(src, drag, row, scale, weight, low_edge, high_edge):
    alpha = weight * scale
    here, below, above, right, left = [], [], [], [], []
    for field in range(3):
        here.append([src[field, half, pl.ds(row, 8), :] for half in (0, 1)])
        below.append([src[field, half, pl.ds(row + 1, 8), :] for half in (0, 1)])
        above.append([src[field, half, pl.ds(row - 1, 8), :] for half in (0, 1)])
        right.append(shifted_lanes(here[field], -1, high_edge))
        left.append(shifted_lanes(here[field], 1, low_edge))
    out = [[], [], []]
    for half in (0, 1):
        e, u, w = (here[field][half] for field in range(3))
        e_ip, u_ip, w_ip = (below[field][half] for field in range(3))
        e_im, u_im, w_im = (above[field][half] for field in range(3))
        e_jp, u_jp, w_jp = (right[field][half] for field in range(3))
        e_jm, u_jm, w_jm = (left[field][half] for field in range(3))
        along = (e_ip - (1.0 + e_ip) * u_ip) + (e_im + (1.0 + e_im) * u_im)
        across = (e_jp - (1.0 + e_jp) * w_jp) + (e_jm + (1.0 + e_jm) * w_jm)
        out[0].append((weight - 4.0 * alpha) * e + alpha * (along + across))
        au = alpha * u
        aw = alpha * w
        u_low, u_high, w_low, w_high = alpha - au, alpha + au, alpha - aw, alpha + aw
        keep = drag[half, pl.ds(row, 8), :]
        out[1].append(
            (u_ip * u_low + u_im * u_high)
            + (u_jp * w_low + u_jm * w_high)
            + ((aw - (2.0 * alpha) * (e_ip - e_im)) + keep * u)
        )
        out[2].append(
            (w_ip * u_low + w_im * u_high)
            + (w_jp * w_low + w_jm * w_high)
            + (keep * w - (au + (2.0 * alpha) * (e_jp - e_jm)))
        )
    return out, here


def kernel(
    times, strips, rows,
    init_ref, guess_ref, fric_ref, c_ref, f_ref,
    first, second, third, fourth, mid, drag_raw, drags, gained, defects, own_defect,
    halo_send, halo_recv, fric_send, fric_recv, init_send, start_recv,
    second_send, second_recv, defect_send, defect_recv, edge_send, edge_recv,
    fourth_send, fourth_recv, hand_send, hand_recv, share_send, met, load_sem,
):
    half = times // 2
    span = math.isqrt(times)
    t = lax.axis_index("tm")
    z = lax.axis_index("space")
    up = lax.rem(z + strips - 1, strips)
    down = lax.rem(z + 1, strips)
    place = lax.rem(t, half)
    slot = lax.rem(t + 2, times)
    slot_place = lax.rem(slot, half)
    hands = t < span
    last = jnp.where(hands, half - 1, place)
    slot_end = slot // half * half + half
    handed = half // span

    own = pl.ds(BASE + HALO, rows)
    upper = pl.ds(BASE, HALO)
    lower = pl.ds(BASE + HALO + rows, HALO)
    own_first = pl.ds(BASE + HALO, HALO)
    own_last = pl.ds(BASE + rows, HALO)

    def remote(src, dst, send, recv, target):
        return pltpu.make_async_remote_copy(
            src_ref=src, dst_ref=dst, send_sem=send, recv_sem=recv, device_id=target, device_id_type=MESH
        )

    def edges_of(ref, send, recv):
        return (
            remote(ref.at[:, :, own_last, :], ref.at[:, :, upper, :], send.at[0], recv.at[0], (t, down)),
            remote(ref.at[:, :, own_first, :], ref.at[:, :, lower, :], send.at[1], recv.at[1], (t, up)),
        )

    barrier = pltpu.get_barrier_semaphore()

    def greet(*target):
        pl.semaphore_signal(barrier, inc=1, device_id=target, device_id_type=MESH)

    greet(t, up)
    greet(t, down)
    partners = []
    for bit in range((times - 1).bit_length()):
        far = 1 << bit
        partners.append(t + far - 2 * far * lax.rem(t // far, 2))
    for partner in partners:
        greet(partner, z)

    is_last = t == times - 1
    is_first = t == times - 2

    def loads(block, ref, turn):
        return [
            pltpu.make_async_copy(
                block.at[..., pl.ds(side * LANES, LANES)], ref.at[:, side, own, :], load_sem.at[turn, side]
            )
            for side in (0, 1)
        ]

    def each_load(act):
        @pl.when(is_last)
        def _():
            for copy in loads(init_ref, first, 0):
                act(copy)

        @pl.when(jnp.logical_not(is_last))
        def _():
            for copy in loads(guess_ref.at[0], first, 0):
                act(copy)

        for side in (0, 1):
            act(
                pltpu.make_async_copy(
                    fric_ref.at[:, pl.ds(side * LANES, LANES)], drag_raw.at[0, side, own, :], load_sem.at[1, side]
                )
            )

        @pl.when(t < half)
        def _():
            for copy in loads(init_ref, third, 2):
                act(copy)

        @pl.when(is_first)
        def _():
            for copy in loads(init_ref, second, 2):
                act(copy)

    each_load(lambda copy: copy.start())
    each_load(lambda copy: copy.wait())
    pl.semaphore_wait(barrier, 2 + len(partners))

    def tell(turn):
        pl.semaphore_signal(met.at[turn], inc=1, device_id=(partners[turn], z), device_id_type=MESH)

    def hear(turn):
        pl.semaphore_wait(met.at[turn], 1)

    tell(0)
    first_edges = edges_of(first, halo_send, halo_recv)
    drag_edges = edges_of(drag_raw, fric_send, fric_recv)
    third_edges = edges_of(third, init_send, start_recv)
    for copy in first_edges + drag_edges:
        copy.start()

    @pl.when(t < half)
    def _():
        for copy in third_edges:
            copy.start()

    lane = lax.broadcasted_iota(jnp.int32, (8, LANES), 1)
    low_edge = lane == 0
    high_edge = lane == LANES - 1
    full = range(BASE, BASE + 2 * HALO + rows, 8)
    inner = range(BASE + 8, BASE + 2 * HALO + rows - 8, 8)
    strip = range(BASE + HALO, BASE + HALO + rows, 8)

    def half_step(state, kind, step, chunks):
        for row in chunks:
            values, _ = advanced(state, drags.at[kind], row, 0.5 * step, 1.0, low_edge, high_edge)
            for field in range(3):
                for side in (0, 1):
                    mid[field, side, pl.ds(row, 8), :] = values[field][side]

    def end_step(state, kind, step, chunks, put):
        for row in chunks:
            values, _ = advanced(mid, drags.at[kind + 1], row, 0.5 * step, 0.5, low_edge, high_edge)
            for field in range(3):
                for side in (0, 1):
                    put(field, side, row, values[field][side] + 0.5 * state[field, side, pl.ds(row, 8), :])

    def heun(state, kind, step, chunks, put):
        half_step(state, kind, step, chunks)
        end_step(state, kind, step, chunks if put is not None else chunks, put)

    def fine_steps(state, count, chunks):
        def put(field, side, row, value):
            state[field, side, pl.ds(row, 8), :] = value

        def step(_, carry):
            heun(state, 0, time_step, chunks, put)
            return carry

        lax.fori_loop(0, count, step, 0)

    for copy in first_edges + drag_edges:
        copy.wait()
    for row in full:
        for side in (0, 1):
            base = 2.0 * drag_raw[0, side, pl.ds(row, 8), :] + 4.0
            for kind, step in ((0, time_step), (2, coarse_step)):
                drags[kind, side, pl.ds(row, 8), :] = 1.0 - (0.5 * step) * base
                drags[kind + 1, side, pl.ds(row, 8), :] = 0.5 - (0.25 * step) * base

    hear(0)
    if len(partners) > 1:
        tell(1)

    fine_steps(first, STEPS - 4, full)
    fine_steps(first, 4, inner)

    @pl.when(jnp.logical_not(is_first))
    def _():
        second[:, :, own, :] = first[:, :, own, :]

    second_edges = edges_of(second, second_send, second_recv)
    for copy in second_edges:
        copy.start()
    if len(partners) > 1:
        hear(1)
    if len(partners) > 2:
        tell(2)
    for copy in second_edges:
        copy.wait_recv()

    half_step(second, 2, coarse_step, inner)

    def put_gain(field, side, row, value):
        gained[field, side, pl.ds(row - BASE - HALO, 8), :] = value

    end_step(second, 2, coarse_step, strip, put_gain)
    if len(partners) > 2:
        hear(2)
    if len(partners) > 3:
        tell(3)
    for copy in second_edges:
        copy.wait_send()
    fine_steps(second, STEPS - 4, full)
    fine_steps(second, 4, inner)
    own_defect[...] = second[:, :, own, :] - gained[...]

    if len(partners) > 3:
        hear(3)
    d_own = pl.ds(HALO, rows)

    slot_low = jnp.maximum(slot, jnp.where(slot < half, span, 0))
    fronts = jnp.where(slot < half, span, 0)

    def each_defect(act):
        def one(turn, carry):
            target = jnp.where(turn < fronts, turn, slot_end - 1 - (turn - fronts))

            @pl.when(target != t)
            def _():
                act(
                    remote(
                        own_defect, defects.at[slot_place, :, :, d_own, :],
                        defect_send.at[turn], defect_recv.at[slot_place], (target, z),
                    )
                )

            return carry

        lax.fori_loop(0, fronts + slot_end - slot_low, one, 0)

    late = slot >= times - 2

    @pl.when(jnp.logical_not(late))
    def _():
        each_defect(lambda copy: copy.start())

    keeps = ((t >= slot_low) & (t < slot_end)) | (t < fronts)

    @pl.when(keeps)
    def _():
        defects[slot_place, :, :, d_own, :] = own_defect[...]

    def each_edge(turn, act):
        need = 2 * (half - 1 - turn)

        def copies(count):
            return (
                remote(
                    defects.at[turn, :, :, pl.ds(HALO + rows - count, count), :],
                    defects.at[turn, :, :, pl.ds(HALO - count, count), :],
                    edge_send.at[0, turn], edge_recv.at[0, turn], (t, down),
                ),
                remote(
                    defects.at[turn, :, :, pl.ds(HALO, count), :],
                    defects.at[turn, :, :, pl.ds(HALO + rows, count), :],
                    edge_send.at[1, turn], edge_recv.at[1, turn], (t, up),
                ),
            )

        @pl.when(need > 8)
        def _():
            for copy in copies(16):
                act(copy)

        @pl.when((need > 0) & (need <= 8))
        def _():
            for copy in copies(8):
                act(copy)

    def pass_edges(turn, carry):
        @pl.when(jnp.logical_not(keeps & (turn == slot_place)))
        def _():
            remote(
                own_defect, defects.at[turn, :, :, d_own, :], defect_send.at[turn], defect_recv.at[turn], (t, z)
            ).wait_recv()

        each_edge(turn, lambda copy: copy.start())
        return carry

    lax.fori_loop(0, last + 1, pass_edges, 0)

    @pl.when(late)
    def _():
        each_defect(lambda copy: copy.start())

    upper_core = lax.rem(z, 2) == 0
    share_down = remote(third.at[:, :, own_last, :], third.at[:, :, upper, :], share_send, start_recv.at[0], (t, down))
    share_up = remote(third.at[:, :, own_first, :], third.at[:, :, lower, :], share_send, start_recv.at[1], (t, up))

    @pl.when(t < half)
    def _():
        for copy in third_edges:
            copy.wait_send()

    @pl.when(t >= half)
    def _():
        remote(third.at[:, :, own, :], third.at[:, :, own, :], hand_send.at[0, 0], hand_recv, (t, z)).wait_recv()

        @pl.when(upper_core)
        def _():
            share_down.start()

        @pl.when(jnp.logical_not(upper_core))
        def _():
            share_up.start()

    for copy in third_edges:
        copy.wait_recv()

    @pl.when((t >= half) & upper_core)
    def _():
        share_down.wait_send()

    @pl.when((t >= half) & jnp.logical_not(upper_core))
    def _():
        share_up.wait_send()

    def chain(chunks):
        def step(turn, carry):
            half_step(third, 2, coarse_step, chunks)
            each_edge(turn, lambda copy: copy.wait_recv())

            def put(field, part, row, value):
                third[field, part, pl.ds(row, 8), :] = value + defects[turn, field, part, pl.ds(row - BASE, 8), :]

            end_step(third, 2, coarse_step, chunks, put)
            return carry

        return step

    wide = max(half - 4, 0)
    lax.fori_loop(0, jnp.minimum(place, wide), chain(full), 0)
    lax.fori_loop(wide, place, chain(inner), 0)

    fourth[:, :, own, :] = third[:, :, own, :]
    fourth_edges = edges_of(fourth, fourth_send, fourth_recv)
    for copy in fourth_edges:
        copy.start()

    def put_out():
        for field in range(3):
            for part in (0, 1):
                c_ref[0, field, :, part * LANES : (part + 1) * LANES] = third[field, part, own, :]

    lax.fori_loop(place, jnp.minimum(place + 1, wide), chain(full), 0)
    lax.fori_loop(jnp.maximum(place, wide), place + 1, chain(inner), 0)
    put_out()
    lax.fori_loop(place + 1, jnp.minimum(last + 1, wide), chain(full), 0)
    lax.fori_loop(jnp.maximum(place + 1, wide), last + 1, chain(inner), 0)

    def each_hand(act):
        def one(turn, carry):
            target = t + times - span - span * turn
            act(remote(third.at[:, :, own, :], third.at[:, :, own, :], hand_send.at[0, turn], hand_recv, (target, z)))

            @pl.when(upper_core)
            def _():
                act(
                    remote(
                        third.at[:, :, own_first, :], third.at[:, :, lower, :],
                        hand_send.at[1, turn], start_recv.at[1], (target, up),
                    )
                )

            @pl.when(jnp.logical_not(upper_core))
            def _():
                act(
                    remote(
                        third.at[:, :, own_last, :], third.at[:, :, upper, :],
                        hand_send.at[1, turn], start_recv.at[0], (target, down),
                    )
                )

            return carry

        lax.fori_loop(0, handed, one, 0)

    @pl.when(hands)
    def _():
        each_hand(lambda copy: copy.start())

    for copy in fourth_edges:
        copy.wait()
    fine_steps(fourth, STEPS - 5, full)
    fine_steps(fourth, 4, inner)
    for field in range(3):
        for side in (0, 1):
            f_ref[0, field, :, side * LANES : (side + 1) * LANES] = fourth[field, side, own, :]

    each_defect(lambda copy: copy.wait_send())

    def sent_edges(turn, carry):
        each_edge(turn, lambda copy: copy.wait_send())
        return carry

    lax.fori_loop(0, last + 1, sent_edges, 0)

    @pl.when(hands)
    def _():
        each_hand(lambda copy: copy.wait_send())


def leave(c_ref, f_ref, c_out, f_out, sem):
    copies = [pltpu.make_async_copy(c_ref, c_out, sem.at[0]), pltpu.make_async_copy(f_ref, f_out, sem.at[1])]
    for copy in copies:
        copy.start()
    for copy in copies:
        copy.wait()


def solution(mesh):
    times, strips = mesh.shape["tm"], mesh.shape["space"]

    def body(initial_state, c_guess, friction):
        rows = friction.shape[0]
        tall = BASE + 2 * HALO + rows + 8
        state = pltpu.VMEM((3, 2, tall, LANES), jnp.float32)
        part = pltpu.VMEM((3, 2, rows, LANES), jnp.float32)
        dma = pltpu.SemaphoreType.DMA
        vmem = pl.BlockSpec(memory_space=pltpu.VMEM)
        shape = pltpu.VMEM(c_guess.shape, jnp.float32)
        results = pl.pallas_call(
            functools.partial(kernel, times, strips, rows),
            out_shape=(shape, shape),
            in_specs=[pl.BlockSpec(memory_space=pl.ANY)] * 3,
            out_specs=(vmem, vmem),
            scratch_shapes=[
                state, state,
                state, state, state,
                pltpu.VMEM((1, 2, tall, LANES), jnp.float32),
                pltpu.VMEM((4, 2, tall, LANES), jnp.float32),
                part,
                pltpu.VMEM((times // 2, 3, 2, 2 * HALO + rows, LANES), jnp.float32),
                part,
                dma((2,)), dma((2,)), dma((2,)), dma((2,)), dma((2,)), dma((2,)),
                dma((2,)), dma((2,)), dma((times,)), dma((times,)), dma((2, times)), dma((2, times)),
                dma((2,)), dma((2,)), dma((2, 4)), dma, dma,
                pltpu.SemaphoreType.REGULAR((4,)), dma((3, 2)),
            ],
            compiler_params=pltpu.CompilerParams(collective_id=0, has_side_effects=True),
            cost_estimate=pl.CostEstimate(flops=100_000_000, bytes_accessed=1_000_000, transcendentals=0),
        )(initial_state, c_guess, friction)
        whole = jax.ShapeDtypeStruct(c_guess.shape, jnp.float32)
        hbm = pl.BlockSpec(memory_space=pl.ANY)
        return pl.pallas_call(
            leave, out_shape=(whole, whole), in_specs=[vmem] * 2, out_specs=(hbm, hbm), scratch_shapes=[dma((2,))]
        )(*[pltpu.with_memory_space_constraint(result, pltpu.VMEM) for result in results])

    return jax.shard_map(
        body,
        mesh=mesh,
        in_specs=(P(None, "space", None), P("tm", None, "space", None), P("space", None)),
        out_specs=(P("tm", None, "space", None), P("tm", None, "space", None)),
        check_vma=False,
    )
```

```python
import functools
import math

import jax
import jax.numpy as jnp
from jax import lax
from jax.experimental import pallas as pl
from jax.experimental.pallas import tpu as pltpu
from jax.sharding import PartitionSpec as P

STEPS = 8
time_step = 0.04
coarse_step = STEPS * time_step
MESH = pl.DeviceIdType.MESH

HALO = 16
LANES = 128
BASE = 8


def shifted_lanes(pair, by, edge):
    turned = [pltpu.roll(part, by % LANES, 1) for part in pair]
    return [jnp.where(edge, turned[1], turned[0]), jnp.where(edge, turned[0], turned[1])]


def advanced(src, drag, row, scale, weight, low_edge, high_edge):
    alpha = weight * scale
    here, below, above, right, left = [], [], [], [], []
    for field in range(3):
        here.append([src[field, half, pl.ds(row, 8), :] for half in (0, 1)])
        below.append([src[field, half, pl.ds(row + 1, 8), :] for half in (0, 1)])
        above.append([src[field, half, pl.ds(row - 1, 8), :] for half in (0, 1)])
        right.append(shifted_lanes(here[field], -1, high_edge))
        left.append(shifted_lanes(here[field], 1, low_edge))
    out = [[], [], []]
    for half in (0, 1):
        e, u, w = (here[field][half] for field in range(3))
        e_ip, u_ip, w_ip = (below[field][half] for field in range(3))
        e_im, u_im, w_im = (above[field][half] for field in range(3))
        e_jp, u_jp, w_jp = (right[field][half] for field in range(3))
        e_jm, u_jm, w_jm = (left[field][half] for field in range(3))
        along = (e_ip - (1.0 + e_ip) * u_ip) + (e_im + (1.0 + e_im) * u_im)
        across = (e_jp - (1.0 + e_jp) * w_jp) + (e_jm + (1.0 + e_jm) * w_jm)
        out[0].append((weight - 4.0 * alpha) * e + alpha * (along + across))
        au = alpha * u
        aw = alpha * w
        u_low, u_high, w_low, w_high = alpha - au, alpha + au, alpha - aw, alpha + aw
        keep = drag[half, pl.ds(row, 8), :]
        out[1].append(
            (u_ip * u_low + u_im * u_high)
            + (u_jp * w_low + u_jm * w_high)
            + ((aw - (2.0 * alpha) * (e_ip - e_im)) + keep * u)
        )
        out[2].append(
            (w_ip * u_low + w_im * u_high)
            + (w_jp * w_low + w_jm * w_high)
            + (keep * w - (au + (2.0 * alpha) * (e_jp - e_jm)))
        )
    return out, here


def kernel(
    times, strips, rows,
    init_ref, guess_ref, fric_ref, c_ref, f_ref,
    first, second, third, fourth, mid, drag_raw, drags, gained, defects, own_defect,
    halo_send, halo_recv, fric_send, fric_recv, init_send, start_recv,
    second_send, second_recv, defect_send, defect_recv, edge_send, edge_recv,
    fourth_send, fourth_recv, hand_send, hand_recv, share_send, met, load_sem,
):
    half = times // 2
    span = math.isqrt(times)
    t = lax.axis_index("tm")
    z = lax.axis_index("space")
    up = lax.rem(z + strips - 1, strips)
    down = lax.rem(z + 1, strips)
    place = lax.rem(t, half)
    slot = lax.rem(t + 2, times)
    slot_place = lax.rem(slot, half)
    hands = t < span
    last = jnp.where(hands, half - 1, place)
    slot_end = slot // half * half + half
    handed = half // span

    own = pl.ds(BASE + HALO, rows)
    upper = pl.ds(BASE, HALO)
    lower = pl.ds(BASE + HALO + rows, HALO)
    own_first = pl.ds(BASE + HALO, HALO)
    own_last = pl.ds(BASE + rows, HALO)

    def remote(src, dst, send, recv, target):
        return pltpu.make_async_remote_copy(
            src_ref=src, dst_ref=dst, send_sem=send, recv_sem=recv, device_id=target, device_id_type=MESH
        )

    def edges_of(ref, send, recv):
        return (
            remote(ref.at[:, :, own_last, :], ref.at[:, :, upper, :], send.at[0], recv.at[0], (t, down)),
            remote(ref.at[:, :, own_first, :], ref.at[:, :, lower, :], send.at[1], recv.at[1], (t, up)),
        )

    barrier = pltpu.get_barrier_semaphore()

    def greet(*target):
        pl.semaphore_signal(barrier, inc=1, device_id=target, device_id_type=MESH)

    greet(t, up)
    greet(t, down)
    partners = []
    for bit in range((times - 1).bit_length()):
        far = 1 << bit
        partners.append(t + far - 2 * far * lax.rem(t // far, 2))
    for partner in partners:
        greet(partner, z)

    is_last = t == times - 1
    is_first = t == times - 2

    def loads(block, ref, turn):
        return [
            pltpu.make_async_copy(
                block.at[..., pl.ds(side * LANES, LANES)], ref.at[:, side, own, :], load_sem.at[turn, side]
            )
            for side in (0, 1)
        ]

    def each_load(act):
        @pl.when(is_last)
        def _():
            for copy in loads(init_ref, first, 0):
                act(copy)

        @pl.when(jnp.logical_not(is_last))
        def _():
            for copy in loads(guess_ref.at[0], first, 0):
                act(copy)

        for side in (0, 1):
            act(
                pltpu.make_async_copy(
                    fric_ref.at[:, pl.ds(side * LANES, LANES)], drag_raw.at[0, side, own, :], load_sem.at[1, side]
                )
            )

    def each_late_load(act):
        @pl.when(t < half)
        def _():
            for copy in loads(init_ref, third, 2):
                act(copy)

        @pl.when(is_first)
        def _():
            for copy in loads(init_ref, second, 2):
                act(copy)

    each_load(lambda copy: copy.start())
    each_late_load(lambda copy: copy.start())
    each_load(lambda copy: copy.wait())
    pl.semaphore_wait(barrier, 2 + len(partners))

    def tell(turn):
        pl.semaphore_signal(met.at[turn], inc=1, device_id=(partners[turn], z), device_id_type=MESH)

    def hear(turn):
        pl.semaphore_wait(met.at[turn], 1)

    tell(0)
    first_edges = edges_of(first, halo_send, halo_recv)
    drag_edges = edges_of(drag_raw, fric_send, fric_recv)
    third_edges = edges_of(third, init_send, start_recv)
    for copy in first_edges + drag_edges:
        copy.start()
    each_late_load(lambda copy: copy.wait())

    @pl.when(t < half)
    def _():
        for copy in third_edges:
            copy.start()

    lane = lax.broadcasted_iota(jnp.int32, (8, LANES), 1)
    low_edge = lane == 0
    high_edge = lane == LANES - 1
    full = range(BASE, BASE + 2 * HALO + rows, 8)
    inner = range(BASE + 8, BASE + 2 * HALO + rows - 8, 8)
    strip = range(BASE + HALO, BASE + HALO + rows, 8)

    def half_step(state, kind, step, chunks):
        for row in chunks:
            values, _ = advanced(state, drags.at[kind], row, 0.5 * step, 1.0, low_edge, high_edge)
            for field in range(3):
                for side in (0, 1):
                    mid[field, side, pl.ds(row, 8), :] = values[field][side]

    def end_step(state, kind, step, chunks, put):
        for row in chunks:
            values, _ = advanced(mid, drags.at[kind + 1], row, 0.5 * step, 0.5, low_edge, high_edge)
            for field in range(3):
                for side in (0, 1):
                    put(field, side, row, values[field][side] + 0.5 * state[field, side, pl.ds(row, 8), :])

    def heun(state, kind, step, chunks, put):
        half_step(state, kind, step, chunks)
        end_step(state, kind, step, chunks if put is not None else chunks, put)

    def fine_steps(state, count, chunks):
        def put(field, side, row, value):
            state[field, side, pl.ds(row, 8), :] = value

        def step(_, carry):
            heun(state, 0, time_step, chunks, put)
            return carry

        lax.fori_loop(0, count, step, 0)

    def last_steps(state):
        fine_steps(state, 3, inner)

        def put(field, side, row, value):
            state[field, side, pl.ds(row, 8), :] = value

        half_step(state, 0, time_step, inner)
        end_step(state, 0, time_step, strip, put)

    def set_drags(chunks):
        for row in chunks:
            for side in (0, 1):
                base = 2.0 * drag_raw[0, side, pl.ds(row, 8), :] + 4.0
                for kind, step in ((0, time_step), (2, coarse_step)):
                    drags[kind, side, pl.ds(row, 8), :] = 1.0 - (0.5 * step) * base
                    drags[kind + 1, side, pl.ds(row, 8), :] = 0.5 - (0.25 * step) * base

    set_drags(strip)
    for copy in first_edges + drag_edges:
        copy.wait()
    set_drags([row for row in full if row not in strip])
    hear(0)
    if len(partners) > 1:
        tell(1)

    fine_steps(first, STEPS - 4, full)
    last_steps(first)

    @pl.when(jnp.logical_not(is_first))
    def _():
        second[:, :, own, :] = first[:, :, own, :]

    second_edges = edges_of(second, second_send, second_recv)
    for copy in second_edges:
        copy.start()
    if len(partners) > 1:
        hear(1)
    if len(partners) > 2:
        tell(2)
    for copy in second_edges:
        copy.wait_recv()

    half_step(second, 2, coarse_step, inner)

    def put_gain(field, side, row, value):
        gained[field, side, pl.ds(row - BASE - HALO, 8), :] = value

    end_step(second, 2, coarse_step, strip, put_gain)
    if len(partners) > 2:
        hear(2)
    if len(partners) > 3:
        tell(3)
    for copy in second_edges:
        copy.wait_send()
    fine_steps(second, STEPS - 4, full)
    last_steps(second)
    own_defect[...] = second[:, :, own, :] - gained[...]

    if len(partners) > 3:
        hear(3)
    d_own = pl.ds(HALO, rows)

    slot_low = jnp.maximum(slot, jnp.where(slot < half, span, 0))
    fronts = jnp.where(slot < half, span, 0)

    def each_defect(act):
        def one(turn, carry):
            target = jnp.where(turn < fronts, turn, slot_end - 1 - (turn - fronts))

            @pl.when(target != t)
            def _():
                act(
                    remote(
                        own_defect, defects.at[slot_place, :, :, d_own, :],
                        defect_send.at[turn], defect_recv.at[slot_place], (target, z),
                    )
                )

            return carry

        lax.fori_loop(0, fronts + slot_end - slot_low, one, 0)

    late = slot >= times - 2

    @pl.when(jnp.logical_not(late))
    def _():
        each_defect(lambda copy: copy.start())

    keeps = ((t >= slot_low) & (t < slot_end)) | (t < fronts)

    @pl.when(keeps)
    def _():
        defects[slot_place, :, :, d_own, :] = own_defect[...]

    def each_edge(turn, act):
        need = 2 * (half - 1 - turn)

        def copies(count):
            return (
                remote(
                    defects.at[turn, :, :, pl.ds(HALO + rows - count, count), :],
                    defects.at[turn, :, :, pl.ds(HALO - count, count), :],
                    edge_send.at[0, turn], edge_recv.at[0, turn], (t, down),
                ),
                remote(
                    defects.at[turn, :, :, pl.ds(HALO, count), :],
                    defects.at[turn, :, :, pl.ds(HALO + rows, count), :],
                    edge_send.at[1, turn], edge_recv.at[1, turn], (t, up),
                ),
            )

        @pl.when(need > 8)
        def _():
            for copy in copies(16):
                act(copy)

        @pl.when((need > 0) & (need <= 8))
        def _():
            for copy in copies(8):
                act(copy)

    def pass_edges(turn, carry):
        @pl.when(jnp.logical_not(keeps & (turn == slot_place)))
        def _():
            remote(
                own_defect, defects.at[turn, :, :, d_own, :], defect_send.at[turn], defect_recv.at[turn], (t, z)
            ).wait_recv()

        each_edge(turn, lambda copy: copy.start())
        return carry

    lax.fori_loop(0, last + 1, pass_edges, 0)

    @pl.when(late)
    def _():
        each_defect(lambda copy: copy.start())

    upper_core = lax.rem(z, 2) == 0
    share_down = remote(third.at[:, :, own_last, :], third.at[:, :, upper, :], share_send, start_recv.at[0], (t, down))
    share_up = remote(third.at[:, :, own_first, :], third.at[:, :, lower, :], share_send, start_recv.at[1], (t, up))

    @pl.when(t < half)
    def _():
        for copy in third_edges:
            copy.wait_send()

    @pl.when(t >= half)
    def _():
        remote(third.at[:, :, own, :], third.at[:, :, own, :], hand_send.at[0, 0], hand_recv, (t, z)).wait_recv()

        @pl.when(upper_core)
        def _():
            share_down.start()

        @pl.when(jnp.logical_not(upper_core))
        def _():
            share_up.start()

    for copy in third_edges:
        copy.wait_recv()

    @pl.when((t >= half) & upper_core)
    def _():
        share_down.wait_send()

    @pl.when((t >= half) & jnp.logical_not(upper_core))
    def _():
        share_up.wait_send()

    def chain(chunks):
        def step(turn, carry):
            half_step(third, 2, coarse_step, chunks)
            each_edge(turn, lambda copy: copy.wait_recv())

            def put(field, part, row, value):
                third[field, part, pl.ds(row, 8), :] = value + defects[turn, field, part, pl.ds(row - BASE, 8), :]

            end_step(third, 2, coarse_step, chunks, put)
            return carry

        return step

    wide = max(half - 4, 0)
    lax.fori_loop(0, jnp.minimum(place, wide), chain(full), 0)
    lax.fori_loop(wide, place, chain(inner), 0)

    fourth[:, :, own, :] = third[:, :, own, :]
    fourth_edges = edges_of(fourth, fourth_send, fourth_recv)
    for copy in fourth_edges:
        copy.start()

    def put_out():
        for field in range(3):
            for part in (0, 1):
                c_ref[0, field, :, part * LANES : (part + 1) * LANES] = third[field, part, own, :]

    lax.fori_loop(place, jnp.minimum(place + 1, wide), chain(full), 0)
    lax.fori_loop(jnp.maximum(place, wide), place + 1, chain(inner), 0)
    put_out()
    lax.fori_loop(place + 1, jnp.minimum(last + 1, wide), chain(full), 0)
    lax.fori_loop(jnp.maximum(place + 1, wide), last + 1, chain(inner), 0)

    def each_hand(act):
        def one(turn, carry):
            target = t + times - span - span * turn
            act(remote(third.at[:, :, own, :], third.at[:, :, own, :], hand_send.at[0, turn], hand_recv, (target, z)))

            @pl.when(upper_core)
            def _():
                act(
                    remote(
                        third.at[:, :, own_first, :], third.at[:, :, lower, :],
                        hand_send.at[1, turn], start_recv.at[1], (target, up),
                    )
                )

            @pl.when(jnp.logical_not(upper_core))
            def _():
                act(
                    remote(
                        third.at[:, :, own_last, :], third.at[:, :, upper, :],
                        hand_send.at[1, turn], start_recv.at[0], (target, down),
                    )
                )

            return carry

        lax.fori_loop(0, handed, one, 0)

    @pl.when(hands)
    def _():
        each_hand(lambda copy: copy.start())

    for copy in fourth_edges:
        copy.wait()
    fine_steps(fourth, STEPS - 5, full)
    last_steps(fourth)
    for field in range(3):
        for side in (0, 1):
            f_ref[0, field, :, side * LANES : (side + 1) * LANES] = fourth[field, side, own, :]

    each_defect(lambda copy: copy.wait_send())

    def sent_edges(turn, carry):
        each_edge(turn, lambda copy: copy.wait_send())
        return carry

    lax.fori_loop(0, last + 1, sent_edges, 0)

    @pl.when(hands)
    def _():
        each_hand(lambda copy: copy.wait_send())


def leave(c_ref, f_ref, c_out, f_out, sem):
    copies = [pltpu.make_async_copy(c_ref, c_out, sem.at[0]), pltpu.make_async_copy(f_ref, f_out, sem.at[1])]
    for copy in copies:
        copy.start()
    for copy in copies:
        copy.wait()


def solution(mesh):
    times, strips = mesh.shape["tm"], mesh.shape["space"]

    def body(initial_state, c_guess, friction):
        rows = friction.shape[0]
        tall = BASE + 2 * HALO + rows + 8
        state = pltpu.VMEM((3, 2, tall, LANES), jnp.float32)
        part = pltpu.VMEM((3, 2, rows, LANES), jnp.float32)
        dma = pltpu.SemaphoreType.DMA
        vmem = pl.BlockSpec(memory_space=pltpu.VMEM)
        shape = pltpu.VMEM(c_guess.shape, jnp.float32)
        results = pl.pallas_call(
            functools.partial(kernel, times, strips, rows),
            out_shape=(shape, shape),
            in_specs=[pl.BlockSpec(memory_space=pl.ANY)] * 3,
            out_specs=(vmem, vmem),
            scratch_shapes=[
                state, state,
                state, state, state,
                pltpu.VMEM((1, 2, tall, LANES), jnp.float32),
                pltpu.VMEM((4, 2, tall, LANES), jnp.float32),
                part,
                pltpu.VMEM((times // 2, 3, 2, 2 * HALO + rows, LANES), jnp.float32),
                part,
                dma((2,)), dma((2,)), dma((2,)), dma((2,)), dma((2,)), dma((2,)),
                dma((2,)), dma((2,)), dma((times,)), dma((times,)), dma((2, times)), dma((2, times)),
                dma((2,)), dma((2,)), dma((2, 4)), dma, dma,
                pltpu.SemaphoreType.REGULAR((4,)), dma((3, 2)),
            ],
            compiler_params=pltpu.CompilerParams(collective_id=0, has_side_effects=True),
            cost_estimate=pl.CostEstimate(flops=100_000_000, bytes_accessed=1_000_000, transcendentals=0),
        )(initial_state, c_guess, friction)
        whole = jax.ShapeDtypeStruct(c_guess.shape, jnp.float32)
        hbm = pl.BlockSpec(memory_space=pl.ANY)
        return pl.pallas_call(
            leave, out_shape=(whole, whole), in_specs=[vmem] * 2, out_specs=(hbm, hbm), scratch_shapes=[dma((2,))]
        )(*[pltpu.with_memory_space_constraint(result, pltpu.VMEM) for result in results])

    return jax.shard_map(
        body,
        mesh=mesh,
        in_specs=(P(None, "space", None), P("tm", None, "space", None), P("space", None)),
        out_specs=(P("tm", None, "space", None), P("tm", None, "space", None)),
        check_vma=False,
    )
```
